32 devices in a mesh: dp: 16 (over z, y, core), mp: 2 (over x).
Axes of the slice: x: 2, y: 2, z: 4, core: 2. Of those that a mesh axis runs over, the one named last changes fastest.
Arguments:
- picture_tower_vectors: bfloat16 [3072, 1152], P('dp'), may hold values from -6 to 6
- caption_tower_vectors: bfloat16 [3072, 1152], P('dp', 'mp'), may hold values from -6 to 6
- picture_standardize_factor: float32 [1152], replicated, may hold values from 0.1 to 1.9
- picture_entry_matrix: bfloat16 [1152, 4304], P(None, 'mp'), may hold values from -0.1875 to 0.1875
- picture_exit_matrix: bfloat16 [4304, 1152], P('mp'), may hold values from -0.09375 to 0.09375
- caption_mapping_matrix: bfloat16 [1152, 1152], P('mp'), may hold values from -1 to 1
- energy_multiplier: float32 [], replicated, may hold values from 4 to 16
- energy_offset_term: float32 [], replicated, may hold values from -2 to -0.5
Outputs:
- grad_image: float32 [3072, 1152], P('dp', 'mp')
- grad_text: float32 [3072, 1152], P('dp', 'mp')
The draws below stay inside these ranges and needn't reach their ends.
All inputs are finite; a program needn't handle non-finite values.
Results may differ from the reference program's by a relative error of at most 0.0046.
Values may be sent and summed in bfloat16 or wider, within the bound.
A program may use at most 64 MiB of HBM per device.

```python
import math
import jax
import jax.numpy as jnp
from jax import lax

D = 1152
FF = 4304
ROWS = 192
PAIRS = 3072
N_DP = 16


def cluster_centres(key):
    anchor_rows = jax.random.normal(jax.random.fold_in(key, 101), (8, D), jnp.float32)
    prototypes = jnp.concatenate([anchor_rows, -anchor_rows], axis=0)
    labels = jax.random.randint(jax.random.fold_in(key, 102), (PAIRS,), 0, 16)
    return prototypes[labels]


def mapping_weights(key):
    entries = jax.random.normal(jax.random.fold_in(key, 103), (D, D), jnp.float32)
    return jnp.clip(entries * (1.0 / math.sqrt(D)), -1.0, 1.0)


def jitter_rows(key):
    return jax.random.normal(key, (PAIRS, D), jnp.float32)


def mix_weights():
    return (0.8, 0.6)


def draw_picture_tower_vectors(key, part):
    centres = cluster_centres(key)
    cluster_weight, jitter_weight = mix_weights()
    values = cluster_weight * centres + jitter_weight * jitter_rows(jax.random.fold_in(key, 104))
    return jnp.clip(values, -6.0, 6.0).astype(jnp.bfloat16)


def draw_caption_tower_vectors(key, part):
    centres = cluster_centres(key)
    mapped = lax.dot_general(centres, mapping_weights(key), (((1,), (1,)), ((), ())), precision=lax.Precision.HIGHEST)
    cluster_weight, jitter_weight = mix_weights()
    values = cluster_weight * mapped + jitter_weight * jitter_rows(jax.random.fold_in(key, 105))
    return jnp.clip(values, -6.0, 6.0).astype(jnp.bfloat16)


def draw_caption_mapping_matrix(key, part):
    return mapping_weights(key).astype(jnp.bfloat16)


def shard_levels(rng, dims, cuts, low, largest):
    level = 1.0
    for axis_at, shards_of in cuts:
        steps = jax.random.uniform(jax.random.fold_in(jax.random.fold_in(rng, 6), axis_at), (shards_of,), jnp.float32, low / len(cuts), largest / len(cuts))
        level = level * jnp.repeat(jnp.exp(steps), dims[axis_at] // shards_of).reshape((-1,) + (1,) * (len(dims) - 1 - axis_at))
    return level


def gaussian(own_key, extent, scale, most, pieces=(), kind=jnp.bfloat16):
    level = shard_levels(own_key, extent, pieces, -0.22, 0.18) if pieces else 1.0
    result = jax.random.normal(own_key, extent, jnp.float32) * scale * level
    return jnp.minimum(jnp.maximum(result, -most), most).astype(kind)


def setup_inputs(seed: int = 0) -> dict:
    arg_keys = jax.random.split(jax.random.key(seed), 9)
    return {
        "picture_tower_vectors": draw_picture_tower_vectors(jax.random.fold_in(arg_keys[8], 71), 0),
        "caption_tower_vectors": draw_caption_tower_vectors(jax.random.fold_in(arg_keys[8], 71), 0),
        "picture_standardize_factor": jnp.clip(1.0 + 0.18 * jax.random.normal(arg_keys[2], (D,), jnp.float32), 0.1, 1.9),
        "picture_entry_matrix": gaussian(arg_keys[3], (D, FF), D ** -0.5, 0.1875, ((1, 2),)),
        "picture_exit_matrix": gaussian(arg_keys[4], (FF, D), FF ** -0.5, 0.09375, ((0, 2),)),
        "caption_mapping_matrix": draw_caption_mapping_matrix(jax.random.fold_in(arg_keys[8], 71), 0),
        "energy_multiplier": jnp.clip(jnp.exp(jax.random.uniform(arg_keys[6], (), jnp.float32, math.log(4.0), math.log(16.0))), 4.0, 16.0),
        "energy_offset_term": jnp.clip(jax.random.uniform(arg_keys[7], (), jnp.float32, -2.0, -0.5), -2.0, -0.5),
    }


def gelu_tanh(values):
    return jax.nn.gelu(values, approximate=True)

def norm_back(upstream, unit_rows, inverse):
    unit_float = unit_rows.astype(jnp.float32)
    along = lax.optimization_barrier(jnp.sum(unit_float * upstream, axis=-1, keepdims=True))
    return inverse * (upstream - unit_float * along)

def reference(picture_tower_vectors, caption_tower_vectors, picture_standardize_factor, picture_entry_matrix, picture_exit_matrix, caption_mapping_matrix, energy_multiplier, energy_offset_term):
    image_float = picture_tower_vectors.astype(jnp.float32)
    mean_row = lax.optimization_barrier(jnp.mean(image_float, axis=-1, keepdims=True))
    variance = lax.optimization_barrier(jnp.mean((image_float - mean_row) ** 2, axis=-1, keepdims=True))
    inv_std = lax.rsqrt(variance + 1e-06)
    centred = (image_float - mean_row) * inv_std
    normed = (centred * picture_standardize_factor).astype(jnp.bfloat16)
    preact = jnp.dot(normed, picture_entry_matrix, preferred_element_type=jnp.float32)
    hidden = gelu_tanh(preact).astype(jnp.bfloat16)
    image_out = image_float + jnp.dot(hidden, picture_exit_matrix, preferred_element_type=jnp.float32)
    inv_image = lax.rsqrt(lax.optimization_barrier(jnp.sum(image_out * image_out, axis=-1, keepdims=True)) + 1e-06)
    unit_image = (image_out * inv_image).astype(jnp.bfloat16)
    text_out = jnp.dot(caption_tower_vectors, caption_mapping_matrix, preferred_element_type=jnp.float32)
    inv_text = lax.rsqrt(lax.optimization_barrier(jnp.sum(text_out * text_out, axis=-1, keepdims=True)) + 1e-06)
    unit_text = (text_out * inv_text).astype(jnp.bfloat16)
    total = ROWS * N_DP
    image_ids = jnp.arange(total, dtype=jnp.int32)

    def block_step(image_dir, block_index):
        first = (block_index * ROWS).astype(jnp.int32)
        block_now = lax.dynamic_slice_in_dim(unit_text, first, ROWS, 0)
        text_ids = first + jnp.arange(ROWS, dtype=jnp.int32)
        cosine_matrix = lax.dot_general(block_now, unit_image, (((1,), (1,)), ((), ())), preferred_element_type=jnp.float32)
        couple_energies = energy_multiplier * cosine_matrix + energy_offset_term
        match_polarity = jnp.where(text_ids[:, None] == image_ids[None, :], 1.0, -1.0).astype(jnp.float32)
        polarity_scaled_energies = (energy_multiplier * -match_polarity * jax.nn.sigmoid(-match_polarity * couple_energies)).astype(jnp.bfloat16)
        image_dir = image_dir + lax.dot_general(polarity_scaled_energies, block_now, (((0,), (0,)), ((), ())), preferred_element_type=jnp.float32)
        text_part = jnp.dot(polarity_scaled_energies, unit_image, preferred_element_type=jnp.float32)
        return (image_dir, text_part)
    image_dir, text_parts = lax.scan(block_step, jnp.zeros((total, D), jnp.float32), jnp.arange(N_DP, dtype=jnp.int32))
    text_dir = text_parts.reshape(total, D)
    grad_out = norm_back(image_dir, unit_image, inv_image)
    grad_out_b = grad_out.astype(jnp.bfloat16)
    grad_hidden = lax.dot_general(grad_out_b, picture_exit_matrix, (((1,), (1,)), ((), ())), preferred_element_type=jnp.float32)
    unused, pull_back = jax.vjp(gelu_tanh, preact)
    grad_pre = pull_back(grad_hidden)[0].astype(jnp.bfloat16)
    grad_normed = lax.dot_general(grad_pre, picture_entry_matrix, (((1,), (1,)), ((), ())), preferred_element_type=jnp.float32)
    scaled = grad_normed * picture_standardize_factor
    mean_one = lax.optimization_barrier(jnp.mean(scaled, axis=-1, keepdims=True))
    mean_two = lax.optimization_barrier(jnp.mean(scaled * centred, axis=-1, keepdims=True))
    grad_image = grad_out + inv_std * (scaled - mean_one - centred * mean_two)
    grad_text_out = norm_back(text_dir, unit_text, inv_text).astype(jnp.bfloat16)
    grad_text = lax.dot_general(grad_text_out, caption_mapping_matrix, (((1,), (1,)), ((), ())), preferred_element_type=jnp.float32)
    return (grad_image, grad_text)
```

```python
import functools
import math

import jax
import jax.numpy as jnp
from jax import lax
from jax.experimental import pallas as pl
from jax.experimental.pallas import tpu as pltpu
from jax.sharding import PartitionSpec as P

F32 = jnp.float32
BF16 = jnp.bfloat16
MESH = pl.DeviceIdType.MESH
TILE = 512
ROOT = math.sqrt(2.0 / math.pi)
NT = (((1,), (1,)), ((), ()))
TN = (((0,), (0,)), ((), ()))


def dot(a, b):
    return jnp.dot(a, b, preferred_element_type=F32)


def dot_nt(a, b):
    return lax.dot_general(a, b, NT, preferred_element_type=F32)


def gelu_pair(x):
    square = x * x
    t = jnp.tanh(ROOT * (x + 0.044715 * (square * x)))
    half = 0.5 * (1.0 + t)
    slope = half + 0.5 * x * (1.0 - t * t) * (ROOT * (1.0 + 0.134145 * square))
    return x * half, slope


def norm_back(upstream, unit_rows, inverse):
    unit_float = unit_rows.astype(F32)
    along = jnp.sum(unit_float * upstream, axis=-1, keepdims=True)
    return inverse * (upstream - unit_float * along)


def body(
    n,
    heads,
    pic_hbm,
    cap_hbm,
    gain_ref,
    entry_hbm,
    exit_hbm,
    map_hbm,
    scale_ref,
    shift_ref,
    out_go,
    out_rest,
    out_text,
    pic,
    cap,
    entry,
    exit_,
    mapping,
    load_sem,
    normed,
    values,
    slope,
    weights,
    acc,
    own_f32,
    parts,
    lands,
    fulls,
    ring_text,
    ring_image,
    gains,
    centres,
    norm_own,
    norm_part,
    norm_land,
    sums_part,
    sums_land,
    part_send,
    part_recv,
    full_send,
    full_recv,
    norm_send,
    norm_recv,
    sums_send,
    sums_recv,
    ring_send,
    ring_recv,
):
    rows, width = pic.shape
    share = rows // heads
    hidden = exit_.shape[0]
    cols = width // heads
    me = lax.axis_index("dp")
    head = lax.axis_index("mp")
    length = n // 4

    def place(index):
        z = index // 4
        y = (index // 2) % 2
        return 2 * (z * (1 - y) + (2 * length - 1 - z) * y) + index % 2

    def device(position):
        position = (position + n) % n
        chip = position // 2
        y = chip // length
        z = chip * (1 - y) + (2 * length - 1 - chip) * y
        return (z * 2 + y) * 2 + position % 2

    pos = place(me)
    right = device(pos + 1)
    left = device(pos - 1)
    forward = n // 2
    backward = n - 1 - forward

    loads = []
    for at, (src, dst) in enumerate(
        (
            (cap_hbm, cap),
            (map_hbm, mapping),
            (pic_hbm, pic),
            (entry_hbm, entry),
            (exit_hbm, exit_),
        )
    ):
        copy = pltpu.make_async_copy(src, dst, load_sem.at[at])
        copy.start()
        loads.append(copy)

    barrier = pltpu.get_barrier_semaphore()
    for neighbour in (left, right):
        pl.semaphore_signal(barrier, inc=1, device_id={"dp": neighbour}, device_id_type=MESH)
    for o in range(1, heads):
        pl.semaphore_signal(
            barrier, inc=1, device_id={"mp": (head + o) % heads}, device_id_type=MESH
        )

    def ring_copy(which, buf, way, step):
        block = device(pos - step if way == 0 else pos + step)
        return pltpu.make_async_remote_copy(
            src_ref=buf.at[block],
            dst_ref=buf.at[block],
            send_sem=ring_send.at[which, way, step],
            recv_sem=ring_recv.at[which, way, step],
            device_id={"dp": right if way == 0 else left},
            device_id_type=MESH,
        )

    def ring_start(which, buf, step):
        if step < forward:
            ring_copy(which, buf, 0, step).start()
        if step < backward:
            ring_copy(which, buf, 1, step).start()

    def ring_next(which, buf, step):
        for way, count in ((0, forward), (1, backward)):
            if step < count:
                block = device(pos - step - 1 if way == 0 else pos + step + 1)
                pltpu.make_async_remote_copy(
                    src_ref=buf.at[block],
                    dst_ref=buf.at[block],
                    send_sem=ring_send.at[which, way, step],
                    recv_sem=ring_recv.at[which, way, step],
                    device_id={"dp": right if way == 0 else left},
                    device_id_type=MESH,
                ).wait_recv()
                if step + 1 < count:
                    ring_copy(which, buf, way, step + 1).start()

    def ring_end(which, buf):
        for way, count in ((0, forward), (1, backward)):
            for step in range(count):
                ring_copy(which, buf, way, step).wait_send()

    def exchange(src, dst, send, recv, spread, span=None):
        def part(ref, at):
            return ref.at[at] if span is None else ref.at[at, :, span]

        copies = []
        for o in range(1, heads):
            to = (head + o) % heads
            source = (head + heads - o) % heads
            sent = pltpu.make_async_remote_copy(
                src_ref=part(src, to if spread else head),
                dst_ref=part(dst, head),
                send_sem=send.at[o],
                recv_sem=recv.at[o],
                device_id={"mp": to},
                device_id_type=MESH,
            )
            got = pltpu.make_async_remote_copy(
                src_ref=part(dst, source),
                dst_ref=part(dst, source),
                send_sem=send.at[o],
                recv_sem=recv.at[o],
                device_id={"mp": to},
                device_id_type=MESH,
            )
            copies.append((sent, got))
        for sent, got in copies:
            sent.start()
        return copies

    def arrived(copies):
        for sent, got in copies:
            got.wait_recv()

    def finished(copies):
        for sent, got in copies:
            sent.wait_send()

    def scatter_start(which, product):
        copies = []
        for at, (first, size) in enumerate(pieces):
            columns = pl.ds(first, size)
            total = product(slice(first, first + size))
            for p in range(heads):
                piece = total[p * share : (p + 1) * share]
                own_f32[p, :, first : first + size] = piece
                parts[which, p, :, first : first + size] = piece.astype(BF16)
            copies += exchange(
                parts.at[which],
                lands.at[which],
                part_send.at[which, at],
                part_recv.at[which, at],
                True,
                columns,
            )
        return copies

    def scatter_sum(which, copies, mine):
        arrived(copies)
        for o in range(1, heads):
            mine = mine + lands[which, (head + heads - o) % heads].astype(F32)
        return mine

    def share_start(which, mine):
        fulls[which, head] = mine
        return exchange(
            fulls.at[which], fulls.at[which], full_send.at[which], full_recv.at[which], False
        )

    def full(which):
        return jnp.concatenate([fulls[which, p] for p in range(heads)], axis=0)

    pending = []
    pieces = [(first, min(TILE, width - first)) for first in range(0, width, TILE)]

    loads[0].wait()
    loads[1].wait()
    pl.semaphore_wait(barrier, 2 + heads - 1)
    text_copies = scatter_start(0, lambda span: dot(cap[...], mapping[:, span]))
    pending.append(text_copies)
    text_mine = own_f32[head]

    loads[2].wait()
    image_float = pic[...].astype(F32)
    mean_row = jnp.mean(image_float, axis=-1, keepdims=True)
    variance = jnp.mean((image_float - mean_row) ** 2, axis=-1, keepdims=True)
    inv_std = lax.rsqrt(variance + 1e-06)
    gain = gain_ref[...].reshape(1, width)
    centred = (image_float - mean_row) * inv_std
    normed[...] = (centred * gain).astype(BF16)
    for p in range(heads):
        gains[p] = gain[:, p * cols : (p + 1) * cols]
        centres[p] = centred[:, p * cols : (p + 1) * cols]

    text_out = scatter_sum(0, text_copies, text_mine)
    inv_text = lax.rsqrt(jnp.sum(text_out * text_out, axis=-1, keepdims=True) + 1e-06)
    unit_text = (text_out * inv_text).astype(BF16)
    ring_text[me] = unit_text
    ring_start(0, ring_text, 0)
    text_full = share_start(0, unit_text)
    pending.append(text_full)

    loads[3].wait()
    loads[4].wait()
    tiles = [(first, min(TILE, hidden - first)) for first in range(0, hidden, TILE)]
    text_steps = iter(range(forward))

    def advance(steps, which, buf, count):
        for _ in range(count):
            step = next(steps, None)
            if step is not None:
                ring_next(which, buf, step)

    for at, (first, size) in enumerate(tiles):
        span = slice(first, first + size)
        value, grad = gelu_pair(dot_nt(normed[...], entry[span, :]))
        slope[:, span] = grad
        values[:, span] = value.astype(BF16)
        if at % 2 == 1:
            advance(text_steps, 0, ring_text, 1)
    image_copies = scatter_start(1, lambda span: dot(values[...], exit_[:, span]))
    pending.append(image_copies)
    mine = own_f32[head] + pic[pl.ds(pl.multiple_of(head * share, 8), share), :].astype(F32)
    advance(text_steps, 0, ring_text, 2)
    image_out = scatter_sum(1, image_copies, mine)
    inv_image = lax.rsqrt(jnp.sum(image_out * image_out, axis=-1, keepdims=True) + 1e-06)
    unit_image = (image_out * inv_image).astype(BF16)
    ring_image[me] = unit_image
    image_full = share_start(1, unit_image)
    pending.append(image_full)
    ring_start(1, ring_image, 0)
    advance(text_steps, 0, ring_text, forward)
    ring_end(0, ring_text)
    arrived(image_full)
    arrived(text_full)

    scale = scale_ref[0, 0]
    shift = shift_ref[0, 0]
    group = 4 if share % 16 == 0 else 1

    def weigh(mine, block, g):
        energy = scale * dot_nt(mine, block) + shift
        shape = (rows, group * share)
        column = lax.broadcasted_iota(jnp.int32, shape, 1)
        ident = column + (g * (group * rows) + head * share)
        for j in range(1, group):
            ident = ident + jnp.where(column >= j * share, rows - share, 0)
        same = ident == lax.broadcasted_iota(jnp.int32, shape, 0) + me * rows
        weight = scale * jax.nn.sigmoid(jnp.where(same, -energy, energy))
        return jnp.where(same, -weight, weight).astype(BF16)

    def terms(rows_ref, buf):
        mine = full(rows_ref)
        if group > 1 and (group * share) % 128 == 0:
            for g in range(n // group):
                block = buf[g * group : (g + 1) * group].reshape(group * share, width)
                weights[:, g * group * share : (g + 1) * group * share] = weigh(mine, block, g)
            return lambda span: dot(
                weights[...], buf[:, :, span].reshape(n * share, span.stop - span.start)
            )
        acc[...] = jnp.zeros_like(acc)

        def one(g, carry):
            block = buf[g] if group == 1 else buf[pl.ds(g * group, group)].reshape(group * share, width)
            acc[...] += dot(weigh(full(rows_ref), block, g), block)
            return carry

        lax.fori_loop(0, n // group, one, 0)
        return lambda span: acc[:, span]

    image_steps = iter(range(forward))
    dir_copies = scatter_start(2, terms(1, ring_text))
    pending.append(dir_copies)
    dir_mine = own_f32[head]
    advance(image_steps, 1, ring_image, 4)
    image_dir = scatter_sum(2, dir_copies, dir_mine)
    grad_out = norm_back(image_dir, fulls[1, head], inv_image)
    grad_full = share_start(2, grad_out.astype(BF16))
    pending.append(grad_full)
    advance(image_steps, 1, ring_image, forward)
    ring_end(1, ring_image)

    dirs_copies = scatter_start(3, terms(0, ring_image))
    pending.append(dirs_copies)
    dirs_mine = own_f32[head]

    arrived(grad_full)
    for p in range(heads):
        out_go[p * share : (p + 1) * share] = fulls[2, p]
    grad_b = full(2)
    for at, (first, size) in enumerate(tiles):
        span = slice(first, first + size)
        values[:, span] = (dot_nt(grad_b, exit_[span, :]) * slope[:, span]).astype(BF16)
    total = dot(values[...], entry[...])
    for p in range(heads):
        piece = total[:, p * cols : (p + 1) * cols]
        norm_own[p] = piece
        norm_part[p] = piece.astype(BF16)
    norm_copies = exchange(norm_part, norm_land, norm_send, norm_recv, True)
    scaled = total * gain_ref[...].reshape(1, width)
    one_sum = jnp.sum(scaled, axis=-1, keepdims=True)
    centred = (pic[...].astype(F32) - mean_row) * inv_std
    two_sum = jnp.sum(scaled * centred, axis=-1, keepdims=True)
    lane = lax.broadcasted_iota(jnp.int32, (rows, 128), 1)
    sums_part[head] = jnp.where(lane == 0, one_sum, two_sum)
    sums_copies = exchange(sums_part, sums_land, sums_send, sums_recv, False)
    pending.append(norm_copies)
    pending.append(sums_copies)

    text_dir = scatter_sum(3, dirs_copies, dirs_mine)
    grad_text_out = norm_back(text_dir, fulls[0, head], inv_text).astype(BF16)
    last_full = share_start(3, grad_text_out)
    pending.append(last_full)

    arrived(norm_copies)
    arrived(sums_copies)
    grad_normed = norm_own[head]
    sums = sums_part[head]
    for o in range(1, heads):
        source = (head + heads - o) % heads
        grad_normed = grad_normed + norm_land[source].astype(F32)
        sums = sums + sums_land[source]
    mean_one = sums[:, 0:1] * (1.0 / width)
    mean_two = sums[:, 1:2] * (1.0 / width)
    centred = centres[head]
    scaled = grad_normed * gains[head]
    out_rest[...] = inv_std * (scaled - mean_one - centred * mean_two)

    arrived(last_full)
    out_text[...] = dot_nt(full(3), mapping[...])
    for copies in pending:
        finished(copies)


def per_device(pic, cap, gain, entry, exit_, mapping, scale, shift):
    rows, width = pic.shape
    n = lax.axis_size("dp")
    heads = lax.axis_size("mp")
    cols = cap.shape[1]
    share = rows // heads
    hidden = entry.shape[1]
    flipped = entry.T
    anywhere = pl.BlockSpec(memory_space=pl.ANY)
    vmem = pl.BlockSpec(memory_space=pltpu.VMEM)
    smem = pl.BlockSpec(memory_space=pltpu.SMEM)
    dma = pltpu.SemaphoreType.DMA
    go, rest, text = pl.pallas_call(
        functools.partial(body, n, heads),
        out_shape=(
            jax.ShapeDtypeStruct((rows, width), BF16),
            jax.ShapeDtypeStruct((rows, cols), F32),
            jax.ShapeDtypeStruct((rows, mapping.shape[0]), F32),
        ),
        in_specs=[anywhere, anywhere, vmem, anywhere, anywhere, anywhere, smem, smem],
        out_specs=(vmem, vmem, vmem),
        scratch_shapes=[
            pltpu.VMEM(pic.shape, BF16),
            pltpu.VMEM(cap.shape, BF16),
            pltpu.VMEM(flipped.shape, BF16),
            pltpu.VMEM(exit_.shape, BF16),
            pltpu.VMEM(mapping.shape, BF16),
            dma((5,)),
            pltpu.VMEM((rows, width), BF16),
            pltpu.VMEM((rows, hidden), BF16),
            pltpu.VMEM((rows, hidden), F32),
            pltpu.VMEM((rows, n * share), BF16),
            pltpu.VMEM((rows, width), F32),
            pltpu.VMEM((heads, share, width), F32),
            pltpu.VMEM((4, heads, share, width), BF16),
            pltpu.VMEM((4, heads, share, width), BF16),
            pltpu.VMEM((4, heads, share, width), BF16),
            pltpu.VMEM((n, share, width), BF16),
            pltpu.VMEM((n, share, width), BF16),
            pltpu.VMEM((heads, 1, cols), F32),
            pltpu.VMEM((heads, rows, cols), F32),
            pltpu.VMEM((heads, rows, cols), F32),
            pltpu.VMEM((heads, rows, cols), BF16),
            pltpu.VMEM((heads, rows, cols), BF16),
            pltpu.VMEM((heads, rows, 128), F32),
            pltpu.VMEM((heads, rows, 128), F32),
            dma((4, pl.cdiv(width, TILE), heads)),
            dma((4, pl.cdiv(width, TILE), heads)),
            dma((4, heads)),
            dma((4, heads)),
            dma((heads,)),
            dma((heads,)),
            dma((heads,)),
            dma((heads,)),
            dma((2, 2, n // 2)),
            dma((2, 2, n // 2)),
        ],
        compiler_params=pltpu.CompilerParams(
            collective_id=0, has_side_effects=True, vmem_limit_bytes=60 * 2**20
        ),
        name="contrastive",
    )(
        pic,
        cap,
        gain,
        flipped,
        exit_,
        mapping,
        scale.reshape(1, 1),
        shift.reshape(1, 1),
    )
    first = lax.axis_index("mp") * cols
    grad_image = lax.dynamic_slice_in_dim(go, first, cols, 1).astype(F32) + rest
    return grad_image, text


def flipped_bit(index, bit):
    return index + bit * (1 - 2 * ((index // bit) % 2))


def dot_tn(a, b):
    return lax.dot_general(a, b, TN, preferred_element_type=F32)


def split_three(x):
    high = x.astype(BF16)
    rest = x - high.astype(F32)
    middle = rest.astype(BF16)
    return high, middle, (rest - middle.astype(F32)).astype(BF16)


def square_body(
    pic_hbm,
    cap_hbm,
    gain_ref,
    entry_hbm,
    exit_hbm,
    map_hbm,
    scale_ref,
    shift_ref,
    out_image,
    out_text,
    pic,
    cap,
    entry,
    exit_,
    mapping,
    load_sem,
    normed,
    centred_ref,
    values,
    slope,
    t_own,
    t_part,
    t_land,
    i_own,
    i_part,
    i_land,
    tbuf,
    ibuf,
    weights,
    d_own,
    d_part,
    d_land,
    g_part,
    g_land,
    s_own,
    c_part,
    c_land,
    y_part,
    y_land,
    h_part,
    h_land,
    gt_part,
    gt_land,
    n_part,
    n_land,
    send_sem,
    recv_sem,
):
    rows, width = pic.shape
    share = rows // 2
    hidden = exit_.shape[0]
    cols = width // 2
    me = lax.axis_index("dp")
    head = lax.axis_index("mp")
    other = 1 - head
    by_core = {"dp": flipped_bit(me, 1)}
    by_y = {"dp": flipped_bit(me, 2)}
    by_low = {"dp": flipped_bit(me, 4)}
    by_high = {"dp": flipped_bit(me, 8)}
    by_x = {"mp": other}
    by_both = {"dp": flipped_bit(me, 4), "mp": other}
    own_rows = pl.ds(pl.multiple_of(head * share, 16), share)
    other_rows = pl.ds(pl.multiple_of(other * share, 16), share)
    top = pl.ds(0, share)
    bottom = pl.ds(share, share)
    tiles = [(first, min(TILE, hidden - first)) for first in range(0, hidden, TILE)]
    piece = width // 3 if width % 384 == 0 else width
    spans = [slice(first, first + piece) for first in range(0, width, piece)]

    load_count = 0

    def load(src, dst):
        nonlocal load_count
        copy = pltpu.make_async_copy(src, dst, load_sem.at[load_count])
        load_count += 1
        copy.start()
        return copy

    cap_loads = [
        load(cap_hbm.at[own_rows], cap.at[top]),
        load(cap_hbm.at[other_rows], cap.at[bottom]),
        load(map_hbm, mapping),
    ]
    pic_loads = [
        load(pic_hbm.at[own_rows], pic.at[top]),
        load(pic_hbm.at[other_rows], pic.at[bottom]),
    ]
    entry_loads = [
        load(entry_hbm.at[pl.ds(first, size)], entry.at[pl.ds(first, size)]) for first, size in tiles
    ]
    exit_loads = [
        load(exit_hbm.at[pl.ds(first, size)], exit_.at[pl.ds(first, size)]) for first, size in tiles
    ]

    barrier = pltpu.get_barrier_semaphore()
    partners = (by_x, by_y, by_high, by_low, by_both, by_core)
    for partner in partners:
        pl.semaphore_signal(barrier, inc=1, device_id=partner, device_id_type=MESH)

    pending = []

    def push(src, dst, partner):
        at = len(pending)
        copy = pltpu.make_async_remote_copy(
            src_ref=src,
            dst_ref=dst,
            send_sem=send_sem.at[at],
            recv_sem=recv_sem.at[at],
            device_id=partner,
            device_id_type=MESH,
        )
        copy.start()
        pending.append(copy)
        return copy

    def arrived(copies):
        for copy in copies:
            copy.wait_recv()

    def slot(ref, at, span=slice(None)):
        return ref.at[pl.ds(at * share, share), span]

    for copy in cap_loads:
        copy.wait()
    text_partials = []
    for at, span in enumerate(spans):
        total = dot(cap[...], mapping[:, span])
        t_own[:, span] = total[:share]
        t_part[:, span] = total[share:].astype(BF16)
        if at == 0:
            pl.semaphore_wait(barrier, len(partners))
        text_partials.append(push(t_part.at[:, span], t_land.at[:, span], by_x))

    for copy in pic_loads:
        copy.wait()
    image_float = pic[...].astype(F32)
    mean_row = jnp.mean(image_float, axis=-1, keepdims=True)
    variance = jnp.mean((image_float - mean_row) ** 2, axis=-1, keepdims=True)
    inv_std = lax.rsqrt(variance + 1e-06)
    gain = gain_ref[...].reshape(1, width)
    centred = (image_float - mean_row) * inv_std
    centred_ref[...] = centred
    normed[...] = (centred * gain).astype(BF16)

    for (first, size), copy in zip(tiles, entry_loads):
        copy.wait()
        span = slice(first, first + size)
        value, grad = gelu_pair(dot_nt(normed[...], entry[span, :]))
        slope[:, span] = grad
        values[:, span] = value.astype(BF16)
    for copy in exit_loads:
        copy.wait()
    image_partials = []
    for span in spans:
        total = dot(values[...], exit_[:, span])
        i_own[:, span] = total[:share] + pic[:share, span].astype(F32)
        i_part[:, span] = total[share:].astype(BF16)
        image_partials.append(push(i_part.at[:, span], i_land.at[:, span], by_x))

    arrived(text_partials)
    text_out = t_own[...] + t_land[...].astype(F32)
    inv_text = lax.rsqrt(jnp.sum(text_out * text_out, axis=-1, keepdims=True) + 1e-06)
    tbuf[:share] = (text_out * inv_text).astype(BF16)
    high_copies = [push(slot(tbuf, 0, span), slot(tbuf, 4, span), by_high) for span in spans]
    y_copy = push(slot(tbuf, 0), slot(tbuf, 2), by_y)
    core_copies = [push(slot(tbuf, 0), slot(tbuf, 1), by_core)]

    arrived(image_partials)
    image_out = i_own[...] + i_land[...].astype(F32)
    inv_image = lax.rsqrt(jnp.sum(image_out * image_out, axis=-1, keepdims=True) + 1e-06)
    ibuf[:share] = (image_out * inv_image).astype(BF16)
    image_copies = [
        push(slot(ibuf, 0), slot(ibuf, 3), by_both),
        push(slot(ibuf, 0), slot(ibuf, 1), by_x),
        push(slot(ibuf, 0), slot(ibuf, 2), by_low),
    ]

    diagonal_copies = []
    for copy, span in zip(high_copies, spans):
        copy.wait_recv()
        diagonal_copies.append(push(slot(tbuf, 4, span), slot(tbuf, 6, span), by_y))
        core_copies.append(push(slot(tbuf, 4, span), slot(tbuf, 5, span), by_core))
    y_copy.wait_recv()
    core_copies.append(push(slot(tbuf, 2), slot(tbuf, 3), by_core))
    for copy, span in zip(diagonal_copies, spans):
        copy.wait_recv()
        core_copies.append(push(slot(tbuf, 6, span), slot(tbuf, 7, span), by_core))
    arrived(core_copies)
    arrived(image_copies)

    scale = scale_ref[0, 0]
    shift = shift_ref[0, 0]
    texts = 8 * share
    group = texts // 3 if texts % 384 == 0 else texts
    for first in range(0, texts, group):
        energy = scale * dot_nt(ibuf[...], tbuf[first : first + group, :]) + shift
        row = lax.broadcasted_iota(jnp.int32, energy.shape, 0)
        column = lax.broadcasted_iota(jnp.int32, energy.shape, 1) + first
        same = jnp.logical_and(row == column, row < share)
        weight = scale * jax.nn.sigmoid(jnp.where(same, -energy, energy))
        weights[:, first : first + group] = jnp.where(same, -weight, weight).astype(BF16)

    dir_copies = []
    for span in spans:
        total = dot(weights[...], tbuf[:, span])
        d_own[:, span] = total[:share]
        d_part[:, span] = total[share:].astype(BF16)
        for at, partner in ((2, by_both), (0, by_x), (1, by_low)):
            dir_copies.append(push(slot(d_part, at, span), slot(d_land, at, span), partner))

    core_copies = []
    for span in spans:
        total = dot_tn(weights[...], ibuf[:, span])
        for at in range(4):
            first = 2 * at * share
            s_own[at, :, span] = total[first : first + share]
            c_part[at * share : (at + 1) * share, span] = total[
                first + share : first + 2 * share
            ].astype(BF16)
        core_copies.append(push(c_part.at[:, span], c_land.at[:, span], by_core))
    diagonal_copies = []
    for copy, span in zip(core_copies, spans):
        copy.wait_recv()
        for at in range(4):
            total = s_own[at, :, span] + c_land[at * share : (at + 1) * share, span].astype(F32)
            if at % 2:
                first = (at // 2) * share
                y_part[first : first + share, span] = total.astype(BF16)
            else:
                s_own[at, :, span] = total
        diagonal_copies.append(push(slot(y_part, 1, span), slot(y_land, 1, span), by_y))
    y_copies = [push(slot(y_part, 0, span), slot(y_land, 0, span), by_y) for span in spans]
    high_copies = []
    for copy, span in zip(diagonal_copies, spans):
        copy.wait_recv()
        h_part[:, span] = (s_own[2, :, span] + y_land[share:, span].astype(F32)).astype(BF16)
        high_copies.append(push(h_part.at[:, span], h_land.at[:, span], by_high))

    arrived(dir_copies)
    image_dir = d_own[...]
    for at in range(3):
        image_dir = image_dir + d_land[at * share : (at + 1) * share, :].astype(F32)
    grad_out = norm_back(image_dir, ibuf[:share], inv_image)
    g_part[...] = grad_out.astype(BF16)
    grad_copy = push(g_part, g_land, by_x)

    grad_copy.wait_recv()
    grad_b = jnp.concatenate([g_part[...], g_land[...]], axis=0)
    for first, size in tiles:
        span = slice(first, first + size)
        values[:, span] = (dot_nt(grad_b, exit_[span, :]) * slope[:, span]).astype(BF16)
    total = dot(values[...], entry[...])
    mine_first = head == 0
    lower = total[:, :cols]
    upper = total[:, cols:]
    theirs = jnp.where(mine_first, upper, lower).astype(BF16)
    n_part[:share, :cols] = theirs[share:]
    n_part[share:, :cols] = theirs[:share]
    grad_normed = jnp.where(mine_first, lower, upper)
    scaled = total * gain_ref[...].reshape(1, width)
    centred = centred_ref[...]
    one_sum = jnp.sum(scaled, axis=-1, keepdims=True)
    two_sum = jnp.sum(scaled * centred, axis=-1, keepdims=True)
    lane = lax.broadcasted_iota(jnp.int32, (rows, n_part.shape[1] - cols), 1)
    packed = jnp.zeros(lane.shape, F32)
    for at, term in enumerate(split_three(one_sum) + split_three(two_sum)):
        packed = jnp.where(lane == at, term.astype(F32), packed)
    n_part[:share, cols:] = packed[share:].astype(BF16)
    n_part[share:, cols:] = packed[:share].astype(BF16)
    norm_copy = push(n_part, n_land, by_x)

    arrived(y_copies)
    arrived(high_copies)
    text_dir = s_own[0] + y_land[:share, :].astype(F32) + h_land[...].astype(F32)
    gt_part[...] = norm_back(text_dir, tbuf[:share], inv_text).astype(BF16)
    text_copy = push(gt_part, gt_land, by_x)

    norm_copy.wait_recv()
    gains = gain_ref[...].reshape(1, width)
    gains = jnp.where(mine_first, gains[:, :cols], gains[:, cols:])
    centred = jnp.where(mine_first, centred[:, :cols], centred[:, cols:])
    grad_float = grad_b.astype(F32)
    grad_float = jnp.where(mine_first, grad_float[:, :cols], grad_float[:, cols:])
    grad_normed = grad_normed + n_land[:, :cols].astype(F32)
    sums = n_land[:, cols:].astype(F32)
    mean_one = (one_sum + (sums[:, 0:1] + sums[:, 1:2] + sums[:, 2:3])) * (1.0 / width)
    mean_two = (two_sum + (sums[:, 3:4] + sums[:, 4:5] + sums[:, 5:6])) * (1.0 / width)
    result = grad_float + inv_std * (grad_normed * gains - mean_one - centred * mean_two)
    out_image[own_rows, :] = result[:share]
    out_image[other_rows, :] = result[share:]

    text_copy.wait_recv()
    result = dot_nt(jnp.concatenate([gt_part[...], gt_land[...]], axis=0), mapping[...])
    out_text[own_rows, :] = result[:share]
    out_text[other_rows, :] = result[share:]
    for copy in pending:
        copy.wait_send()


def square_device(pic, cap, gain, entry, exit_, mapping, scale, shift):
    rows, width = pic.shape
    cols = cap.shape[1]
    share = rows // 2
    hidden = entry.shape[1]
    flipped = entry.T
    anywhere = pl.BlockSpec(memory_space=pl.ANY)
    vmem = pl.BlockSpec(memory_space=pltpu.VMEM)
    smem = pl.BlockSpec(memory_space=pltpu.SMEM)
    dma = pltpu.SemaphoreType.DMA

    def blocks(count, dtype=BF16):
        return pltpu.VMEM((count * share, width), dtype)

    loads = 5 + 2 * pl.cdiv(hidden, TILE)
    copies = 64
    extended = 128 * (cols // 128 + 1)
    return pl.pallas_call(
        square_body,
        out_shape=(
            jax.ShapeDtypeStruct((rows, cols), F32),
            jax.ShapeDtypeStruct((rows, mapping.shape[0]), F32),
        ),
        in_specs=[anywhere, anywhere, vmem, anywhere, anywhere, anywhere, smem, smem],
        out_specs=(vmem, vmem),
        scratch_shapes=[
            pltpu.VMEM(pic.shape, BF16),
            pltpu.VMEM(cap.shape, BF16),
            pltpu.VMEM(flipped.shape, BF16),
            pltpu.VMEM(exit_.shape, BF16),
            pltpu.VMEM(mapping.shape, BF16),
            dma((loads,)),
            pltpu.VMEM((rows, width), BF16),
            pltpu.VMEM((rows, width), F32),
            pltpu.VMEM((rows, hidden), BF16),
            pltpu.VMEM((rows, hidden), F32),
            blocks(1, F32),
            blocks(1),
            blocks(1),
            blocks(1, F32),
            blocks(1),
            blocks(1),
            blocks(8),
            blocks(4),
            pltpu.VMEM((4 * share, 8 * share), BF16),
            blocks(1, F32),
            blocks(3),
            blocks(3),
            blocks(1),
            blocks(1),
            pltpu.VMEM((4, share, width), F32),
            blocks(4),
            blocks(4),
            blocks(2),
            blocks(2),
            blocks(1),
            blocks(1),
            blocks(1),
            blocks(1),
            pltpu.VMEM((rows, extended), BF16),
            pltpu.VMEM((rows, extended), BF16),
            dma((copies,)),
            dma((copies,)),
        ],
        compiler_params=pltpu.CompilerParams(
            collective_id=0, has_side_effects=True, vmem_limit_bytes=60 * 2**20
        ),
        name="contrastive_square",
    )(
        pic,
        cap,
        gain,
        flipped,
        exit_,
        mapping,
        scale.reshape(1, 1),
        shift.reshape(1, 1),
    )


def solution(mesh):
    in_specs = (
        P("dp", None),
        P("dp", "mp"),
        P(),
        P(None, "mp"),
        P("mp", None),
        P("mp", None),
        P(),
        P(),
    )
    out_specs = (P("dp", "mp"), P("dp", "mp"))
    square = mesh.shape["mp"] == 2 and mesh.shape["dp"] == 16
    return jax.shard_map(
        square_device if square else per_device, mesh=mesh, in_specs=in_specs, out_specs=out_specs, check_vma=False
    )
```

```python
import functools
import math

import jax
import jax.numpy as jnp
from jax import lax
from jax.experimental import pallas as pl
from jax.experimental.pallas import tpu as pltpu
from jax.sharding import PartitionSpec as P

F32 = jnp.float32
BF16 = jnp.bfloat16
MESH = pl.DeviceIdType.MESH
TILE = 512
ROOT = math.sqrt(2.0 / math.pi)
NT = (((1,), (1,)), ((), ()))
TN = (((0,), (0,)), ((), ()))


def dot(a, b):
    return jnp.dot(a, b, preferred_element_type=F32)


def dot_nt(a, b):
    return lax.dot_general(a, b, NT, preferred_element_type=F32)


def gelu_pair(x):
    square = x * x
    t = jnp.tanh(ROOT * (x + 0.044715 * (square * x)))
    half = 0.5 * (1.0 + t)
    slope = half + 0.5 * x * (1.0 - t * t) * (ROOT * (1.0 + 0.134145 * square))
    return x * half, slope


def norm_back(upstream, unit_rows, inverse):
    unit_float = unit_rows.astype(F32)
    along = jnp.sum(unit_float * upstream, axis=-1, keepdims=True)
    return inverse * (upstream - unit_float * along)


def body(
    n,
    heads,
    pic_hbm,
    cap_hbm,
    gain_ref,
    entry_hbm,
    exit_hbm,
    map_hbm,
    scale_ref,
    shift_ref,
    out_go,
    out_rest,
    out_text,
    pic,
    cap,
    entry,
    exit_,
    mapping,
    load_sem,
    normed,
    values,
    slope,
    weights,
    acc,
    own_f32,
    parts,
    lands,
    fulls,
    ring_text,
    ring_image,
    gains,
    centres,
    norm_own,
    norm_part,
    norm_land,
    sums_part,
    sums_land,
    part_send,
    part_recv,
    full_send,
    full_recv,
    norm_send,
    norm_recv,
    sums_send,
    sums_recv,
    ring_send,
    ring_recv,
):
    rows, width = pic.shape
    share = rows // heads
    hidden = exit_.shape[0]
    cols = width // heads
    me = lax.axis_index("dp")
    head = lax.axis_index("mp")
    length = n // 4

    def place(index):
        z = index // 4
        y = (index // 2) % 2
        return 2 * (z * (1 - y) + (2 * length - 1 - z) * y) + index % 2

    def device(position):
        position = (position + n) % n
        chip = position // 2
        y = chip // length
        z = chip * (1 - y) + (2 * length - 1 - chip) * y
        return (z * 2 + y) * 2 + position % 2

    pos = place(me)
    right = device(pos + 1)
    left = device(pos - 1)
    forward = n // 2
    backward = n - 1 - forward

    loads = []
    for at, (src, dst) in enumerate(
        (
            (cap_hbm, cap),
            (map_hbm, mapping),
            (pic_hbm, pic),
            (entry_hbm, entry),
            (exit_hbm, exit_),
        )
    ):
        copy = pltpu.make_async_copy(src, dst, load_sem.at[at])
        copy.start()
        loads.append(copy)

    barrier = pltpu.get_barrier_semaphore()
    for neighbour in (left, right):
        pl.semaphore_signal(barrier, inc=1, device_id={"dp": neighbour}, device_id_type=MESH)
    for o in range(1, heads):
        pl.semaphore_signal(
            barrier, inc=1, device_id={"mp": (head + o) % heads}, device_id_type=MESH
        )

    def ring_copy(which, buf, way, step):
        block = device(pos - step if way == 0 else pos + step)
        return pltpu.make_async_remote_copy(
            src_ref=buf.at[block],
            dst_ref=buf.at[block],
            send_sem=ring_send.at[which, way, step],
            recv_sem=ring_recv.at[which, way, step],
            device_id={"dp": right if way == 0 else left},
            device_id_type=MESH,
        )

    def ring_start(which, buf, step):
        if step < forward:
            ring_copy(which, buf, 0, step).start()
        if step < backward:
            ring_copy(which, buf, 1, step).start()

    def ring_next(which, buf, step):
        for way, count in ((0, forward), (1, backward)):
            if step < count:
                block = device(pos - step - 1 if way == 0 else pos + step + 1)
                pltpu.make_async_remote_copy(
                    src_ref=buf.at[block],
                    dst_ref=buf.at[block],
                    send_sem=ring_send.at[which, way, step],
                    recv_sem=ring_recv.at[which, way, step],
                    device_id={"dp": right if way == 0 else left},
                    device_id_type=MESH,
                ).wait_recv()
                if step + 1 < count:
                    ring_copy(which, buf, way, step + 1).start()

    def ring_end(which, buf):
        for way, count in ((0, forward), (1, backward)):
            for step in range(count):
                ring_copy(which, buf, way, step).wait_send()

    def exchange(src, dst, send, recv, spread, span=None):
        def part(ref, at):
            return ref.at[at] if span is None else ref.at[at, :, span]

        copies = []
        for o in range(1, heads):
            to = (head + o) % heads
            source = (head + heads - o) % heads
            sent = pltpu.make_async_remote_copy(
                src_ref=part(src, to if spread else head),
                dst_ref=part(dst, head),
                send_sem=send.at[o],
                recv_sem=recv.at[o],
                device_id={"mp": to},
                device_id_type=MESH,
            )
            got = pltpu.make_async_remote_copy(
                src_ref=part(dst, source),
                dst_ref=part(dst, source),
                send_sem=send.at[o],
                recv_sem=recv.at[o],
                device_id={"mp": to},
                device_id_type=MESH,
            )
            copies.append((sent, got))
        for sent, got in copies:
            sent.start()
        return copies

    def arrived(copies):
        for sent, got in copies:
            got.wait_recv()

    def finished(copies):
        for sent, got in copies:
            sent.wait_send()

    def scatter_start(which, product):
        copies = []
        for at, (first, size) in enumerate(pieces):
            columns = pl.ds(first, size)
            total = product(slice(first, first + size))
            for p in range(heads):
                piece = total[p * share : (p + 1) * share]
                own_f32[p, :, first : first + size] = piece
                parts[which, p, :, first : first + size] = piece.astype(BF16)
            copies += exchange(
                parts.at[which],
                lands.at[which],
                part_send.at[which, at],
                part_recv.at[which, at],
                True,
                columns,
            )
        return copies

    def scatter_sum(which, copies, mine):
        arrived(copies)
        for o in range(1, heads):
            mine = mine + lands[which, (head + heads - o) % heads].astype(F32)
        return mine

    def share_start(which, mine):
        fulls[which, head] = mine
        return exchange(
            fulls.at[which], fulls.at[which], full_send.at[which], full_recv.at[which], False
        )

    def full(which):
        return jnp.concatenate([fulls[which, p] for p in range(heads)], axis=0)

    pending = []
    pieces = [(first, min(TILE, width - first)) for first in range(0, width, TILE)]

    loads[0].wait()
    loads[1].wait()
    pl.semaphore_wait(barrier, 2 + heads - 1)
    text_copies = scatter_start(0, lambda span: dot(cap[...], mapping[:, span]))
    pending.append(text_copies)
    text_mine = own_f32[head]

    loads[2].wait()
    image_float = pic[...].astype(F32)
    mean_row = jnp.mean(image_float, axis=-1, keepdims=True)
    variance = jnp.mean((image_float - mean_row) ** 2, axis=-1, keepdims=True)
    inv_std = lax.rsqrt(variance + 1e-06)
    gain = gain_ref[...].reshape(1, width)
    centred = (image_float - mean_row) * inv_std
    normed[...] = (centred * gain).astype(BF16)
    for p in range(heads):
        gains[p] = gain[:, p * cols : (p + 1) * cols]
        centres[p] = centred[:, p * cols : (p + 1) * cols]

    text_out = scatter_sum(0, text_copies, text_mine)
    inv_text = lax.rsqrt(jnp.sum(text_out * text_out, axis=-1, keepdims=True) + 1e-06)
    unit_text = (text_out * inv_text).astype(BF16)
    ring_text[me] = unit_text
    ring_start(0, ring_text, 0)
    text_full = share_start(0, unit_text)
    pending.append(text_full)

    loads[3].wait()
    loads[4].wait()
    tiles = [(first, min(TILE, hidden - first)) for first in range(0, hidden, TILE)]
    text_steps = iter(range(forward))

    def advance(steps, which, buf, count):
        for _ in range(count):
            step = next(steps, None)
            if step is not None:
                ring_next(which, buf, step)

    for at, (first, size) in enumerate(tiles):
        span = slice(first, first + size)
        value, grad = gelu_pair(dot_nt(normed[...], entry[span, :]))
        slope[:, span] = grad
        values[:, span] = value.astype(BF16)
        if at % 2 == 1:
            advance(text_steps, 0, ring_text, 1)
    image_copies = scatter_start(1, lambda span: dot(values[...], exit_[:, span]))
    pending.append(image_copies)
    mine = own_f32[head] + pic[pl.ds(pl.multiple_of(head * share, 8), share), :].astype(F32)
    advance(text_steps, 0, ring_text, 2)
    image_out = scatter_sum(1, image_copies, mine)
    inv_image = lax.rsqrt(jnp.sum(image_out * image_out, axis=-1, keepdims=True) + 1e-06)
    unit_image = (image_out * inv_image).astype(BF16)
    ring_image[me] = unit_image
    image_full = share_start(1, unit_image)
    pending.append(image_full)
    ring_start(1, ring_image, 0)
    advance(text_steps, 0, ring_text, forward)
    ring_end(0, ring_text)
    arrived(image_full)
    arrived(text_full)

    scale = scale_ref[0, 0]
    shift = shift_ref[0, 0]
    group = 4 if share % 16 == 0 else 1

    def weigh(mine, block, g):
        energy = scale * dot_nt(mine, block) + shift
        shape = (rows, group * share)
        column = lax.broadcasted_iota(jnp.int32, shape, 1)
        ident = column + (g * (group * rows) + head * share)
        for j in range(1, group):
            ident = ident + jnp.where(column >= j * share, rows - share, 0)
        same = ident == lax.broadcasted_iota(jnp.int32, shape, 0) + me * rows
        weight = scale * jax.nn.sigmoid(jnp.where(same, -energy, energy))
        return jnp.where(same, -weight, weight).astype(BF16)

    def terms(rows_ref, buf):
        mine = full(rows_ref)
        if group > 1 and (group * share) % 128 == 0:
            for g in range(n // group):
                block = buf[g * group : (g + 1) * group].reshape(group * share, width)
                weights[:, g * group * share : (g + 1) * group * share] = weigh(mine, block, g)
            return lambda span: dot(
                weights[...], buf[:, :, span].reshape(n * share, span.stop - span.start)
            )
        acc[...] = jnp.zeros_like(acc)

        def one(g, carry):
            block = buf[g] if group == 1 else buf[pl.ds(g * group, group)].reshape(group * share, width)
            acc[...] += dot(weigh(full(rows_ref), block, g), block)
            return carry

        lax.fori_loop(0, n // group, one, 0)
        return lambda span: acc[:, span]

    image_steps = iter(range(forward))
    dir_copies = scatter_start(2, terms(1, ring_text))
    pending.append(dir_copies)
    dir_mine = own_f32[head]
    advance(image_steps, 1, ring_image, 4)
    image_dir = scatter_sum(2, dir_copies, dir_mine)
    grad_out = norm_back(image_dir, fulls[1, head], inv_image)
    grad_full = share_start(2, grad_out.astype(BF16))
    pending.append(grad_full)
    advance(image_steps, 1, ring_image, forward)
    ring_end(1, ring_image)

    dirs_copies = scatter_start(3, terms(0, ring_image))
    pending.append(dirs_copies)
    dirs_mine = own_f32[head]

    arrived(grad_full)
    for p in range(heads):
        out_go[p * share : (p + 1) * share] = fulls[2, p]
    grad_b = full(2)
    for at, (first, size) in enumerate(tiles):
        span = slice(first, first + size)
        values[:, span] = (dot_nt(grad_b, exit_[span, :]) * slope[:, span]).astype(BF16)
    total = dot(values[...], entry[...])
    for p in range(heads):
        piece = total[:, p * cols : (p + 1) * cols]
        norm_own[p] = piece
        norm_part[p] = piece.astype(BF16)
    norm_copies = exchange(norm_part, norm_land, norm_send, norm_recv, True)
    scaled = total * gain_ref[...].reshape(1, width)
    one_sum = jnp.sum(scaled, axis=-1, keepdims=True)
    centred = (pic[...].astype(F32) - mean_row) * inv_std
    two_sum = jnp.sum(scaled * centred, axis=-1, keepdims=True)
    lane = lax.broadcasted_iota(jnp.int32, (rows, 128), 1)
    sums_part[head] = jnp.where(lane == 0, one_sum, two_sum)
    sums_copies = exchange(sums_part, sums_land, sums_send, sums_recv, False)
    pending.append(norm_copies)
    pending.append(sums_copies)

    text_dir = scatter_sum(3, dirs_copies, dirs_mine)
    grad_text_out = norm_back(text_dir, fulls[0, head], inv_text).astype(BF16)
    last_full = share_start(3, grad_text_out)
    pending.append(last_full)

    arrived(norm_copies)
    arrived(sums_copies)
    grad_normed = norm_own[head]
    sums = sums_part[head]
    for o in range(1, heads):
        source = (head + heads - o) % heads
        grad_normed = grad_normed + norm_land[source].astype(F32)
        sums = sums + sums_land[source]
    mean_one = sums[:, 0:1] * (1.0 / width)
    mean_two = sums[:, 1:2] * (1.0 / width)
    centred = centres[head]
    scaled = grad_normed * gains[head]
    out_rest[...] = inv_std * (scaled - mean_one - centred * mean_two)

    arrived(last_full)
    out_text[...] = dot_nt(full(3), mapping[...])
    for copies in pending:
        finished(copies)


def per_device(pic, cap, gain, entry, exit_, mapping, scale, shift):
    rows, width = pic.shape
    n = lax.axis_size("dp")
    heads = lax.axis_size("mp")
    cols = cap.shape[1]
    share = rows // heads
    hidden = entry.shape[1]
    flipped = entry.T
    anywhere = pl.BlockSpec(memory_space=pl.ANY)
    vmem = pl.BlockSpec(memory_space=pltpu.VMEM)
    smem = pl.BlockSpec(memory_space=pltpu.SMEM)
    dma = pltpu.SemaphoreType.DMA
    go, rest, text = pl.pallas_call(
        functools.partial(body, n, heads),
        out_shape=(
            jax.ShapeDtypeStruct((rows, width), BF16),
            jax.ShapeDtypeStruct((rows, cols), F32),
            jax.ShapeDtypeStruct((rows, mapping.shape[0]), F32),
        ),
        in_specs=[anywhere, anywhere, vmem, anywhere, anywhere, anywhere, smem, smem],
        out_specs=(vmem, vmem, vmem),
        scratch_shapes=[
            pltpu.VMEM(pic.shape, BF16),
            pltpu.VMEM(cap.shape, BF16),
            pltpu.VMEM(flipped.shape, BF16),
            pltpu.VMEM(exit_.shape, BF16),
            pltpu.VMEM(mapping.shape, BF16),
            dma((5,)),
            pltpu.VMEM((rows, width), BF16),
            pltpu.VMEM((rows, hidden), BF16),
            pltpu.VMEM((rows, hidden), F32),
            pltpu.VMEM((rows, n * share), BF16),
            pltpu.VMEM((rows, width), F32),
            pltpu.VMEM((heads, share, width), F32),
            pltpu.VMEM((4, heads, share, width), BF16),
            pltpu.VMEM((4, heads, share, width), BF16),
            pltpu.VMEM((4, heads, share, width), BF16),
            pltpu.VMEM((n, share, width), BF16),
            pltpu.VMEM((n, share, width), BF16),
            pltpu.VMEM((heads, 1, cols), F32),
            pltpu.VMEM((heads, rows, cols), F32),
            pltpu.VMEM((heads, rows, cols), F32),
            pltpu.VMEM((heads, rows, cols), BF16),
            pltpu.VMEM((heads, rows, cols), BF16),
            pltpu.VMEM((heads, rows, 128), F32),
            pltpu.VMEM((heads, rows, 128), F32),
            dma((4, pl.cdiv(width, TILE), heads)),
            dma((4, pl.cdiv(width, TILE), heads)),
            dma((4, heads)),
            dma((4, heads)),
            dma((heads,)),
            dma((heads,)),
            dma((heads,)),
            dma((heads,)),
            dma((2, 2, n // 2)),
            dma((2, 2, n // 2)),
        ],
        compiler_params=pltpu.CompilerParams(
            collective_id=0, has_side_effects=True, vmem_limit_bytes=60 * 2**20
        ),
        name="contrastive",
    )(
        pic,
        cap,
        gain,
        flipped,
        exit_,
        mapping,
        scale.reshape(1, 1),
        shift.reshape(1, 1),
    )
    first = lax.axis_index("mp") * cols
    grad_image = lax.dynamic_slice_in_dim(go, first, cols, 1).astype(F32) + rest
    return grad_image, text


def flipped_bit(index, bit):
    return index + bit * (1 - 2 * ((index // bit) % 2))


def dot_tn(a, b):
    return lax.dot_general(a, b, TN, preferred_element_type=F32)


def split_three(x):
    high = x.astype(BF16)
    rest = x - high.astype(F32)
    middle = rest.astype(BF16)
    return high, middle, (rest - middle.astype(F32)).astype(BF16)


def square_body(
    pic_hbm,
    cap_hbm,
    gain_hbm,
    entry_hbm,
    exit_hbm,
    map_hbm,
    scale_ref,
    shift_ref,
    out_image,
    out_text,
    pic,
    cap,
    gain_ref,
    entry,
    exit_,
    mapping,
    load_sem,
    normed,
    centred_ref,
    values,
    slope,
    t_own,
    t_part,
    t_land,
    i_own,
    i_part,
    i_land,
    tbuf,
    ibuf,
    weights,
    d_own,
    d_near,
    d_part,
    d_through,
    d_land,
    g_part,
    g_land,
    s_own,
    c_part,
    c_land,
    y_part,
    y_land,
    h_part,
    h_land,
    gt_part,
    gt_land,
    n_part,
    n_land,
    send_sem,
    recv_sem,
):
    rows, width = pic.shape
    share = rows // 2
    hidden = exit_.shape[0]
    cols = width // 2
    me = lax.axis_index("dp")
    head = lax.axis_index("mp")
    other = 1 - head
    by_core = {"dp": flipped_bit(me, 1)}
    by_y = {"dp": flipped_bit(me, 2)}
    by_low = {"dp": flipped_bit(me, 4)}
    by_high = {"dp": flipped_bit(me, 8)}
    by_x = {"mp": other}
    own_rows = pl.ds(pl.multiple_of(head * share, 16), share)
    other_rows = pl.ds(pl.multiple_of(other * share, 16), share)
    tiles = [(first, min(TILE, hidden - first)) for first in range(0, hidden, TILE)]
    chunk = share // 2 if share % 32 == 0 else share
    chunks = range(share // chunk)
    spans = [slice(first, min(first + TILE, width)) for first in range(0, width, TILE)]

    def block(ref, at):
        return ref.at[pl.ds(at * share, share)]

    def part(ref, at, k):
        return ref.at[pl.ds(at * share + k * chunk, chunk)]

    def of(at):
        return slice(at * share, (at + 1) * share)

    def lines(at, k):
        return slice(at * share + k * chunk, at * share + (k + 1) * chunk)

    load_count = 0

    def load(src, dst):
        nonlocal load_count
        copy = pltpu.make_async_copy(src, dst, load_sem.at[load_count])
        load_count += 1
        copy.start()
        return copy

    cap_loads = [
        load(cap_hbm.at[other_rows], block(cap, 1)),
        load(map_hbm, mapping),
        load(cap_hbm.at[own_rows], block(cap, 0)),
    ]
    pic_loads = [
        load(pic_hbm.at[own_rows], block(pic, 0)),
        load(pic_hbm.at[other_rows], block(pic, 1)),
        load(gain_hbm, gain_ref),
    ]
    entry_loads = [
        load(entry_hbm.at[pl.ds(first, size)], entry.at[pl.ds(first, size)]) for first, size in tiles
    ]
    exit_loads = [
        load(exit_hbm.at[pl.ds(first, size)], exit_.at[pl.ds(first, size)]) for first, size in tiles
    ]

    barrier = pltpu.get_barrier_semaphore()
    partners = (by_x, by_y, by_high, by_low, by_core)
    for partner in partners:
        pl.semaphore_signal(barrier, inc=1, device_id=partner, device_id_type=MESH)

    pending = []

    def push(src, dst, partner):
        at = len(pending)
        copy = pltpu.make_async_remote_copy(
            src_ref=src,
            dst_ref=dst,
            send_sem=send_sem.at[at],
            recv_sem=recv_sem.at[at],
            device_id=partner,
            device_id_type=MESH,
        )
        copy.start()
        pending.append(copy)
        return copy

    def arrived(copies):
        for copy in copies:
            copy.wait_recv()

    for copy in cap_loads:
        copy.wait()
    t_part[...] = dot(cap[share:], mapping[...]).astype(BF16)
    pl.semaphore_wait(barrier, len(partners))
    text_partials = [push(part(t_part, 0, k), part(t_land, 0, k), by_x) for k in chunks]
    t_own[...] = dot(cap[:share], mapping[...])

    for copy in pic_loads:
        copy.wait()
    image_float = pic[...].astype(F32)
    mean_row = jnp.mean(image_float, axis=-1, keepdims=True)
    variance = jnp.mean((image_float - mean_row) ** 2, axis=-1, keepdims=True)
    inv_std = lax.rsqrt(variance + 1e-06)
    gain = gain_ref[...].reshape(1, width)
    centred = (image_float - mean_row) * inv_std
    centred_ref[...] = centred
    normed[...] = (centred * gain).astype(BF16)

    for (first, size), copy in zip(tiles, entry_loads):
        copy.wait()
        span = slice(first, first + size)
        value, grad = gelu_pair(dot_nt(normed[...], entry[span, :]))
        slope[:, span] = grad
        values[:, span] = value.astype(BF16)

    def unit_rows(own, land, k, dst):
        total = own[lines(0, k)] + land[lines(0, k)].astype(F32)
        inverse = lax.rsqrt(jnp.sum(total * total, axis=-1, keepdims=True) + 1e-06)
        dst[lines(0, k)] = (total * inverse).astype(BF16)
        return inverse

    inv_text = []
    high_copies = []
    y_copies = []
    core_copies = []

    def text_chunk(k):
        text_partials[k].wait_recv()
        inv_text.append(unit_rows(t_own, t_land, k, tbuf))
        high_copies.append(push(part(tbuf, 0, k), part(tbuf, 2, k), by_high))
        y_copies.append(push(part(tbuf, 0, k), part(tbuf, 1, k), by_y))
        core_copies.append(push(part(tbuf, 0, k), part(tbuf, 4, k), by_core))

    text_chunk(0)
    for copy in exit_loads:
        copy.wait()
    for span in spans:
        i_part[:, span] = dot(values[share:], exit_[:, span]).astype(BF16)
    image_partials = [push(part(i_part, 0, k), part(i_land, 0, k), by_x) for k in chunks]
    for k in chunks[1:]:
        text_chunk(k)
    for span in spans:
        i_own[:, span] = dot(values[:share], exit_[:, span]) + pic[:share, span].astype(F32)

    inv_image = []
    x_copies = []
    low_copies = []
    for k in chunks:
        image_partials[k].wait_recv()
        inv_image.append(unit_rows(i_own, i_land, k, ibuf))
        x_copies.append(push(part(ibuf, 0, k), part(ibuf, 1, k), by_x))
        low_copies.append(push(part(ibuf, 0, k), part(ibuf, 2, k), by_low))

    for k in chunks:
        y_copies[k].wait_recv()
        core_copies.append(push(part(tbuf, 1, k), part(tbuf, 5, k), by_core))
    diagonal_copies = []
    image_diagonals = []
    for k in chunks:
        if k % 2 == 0:
            x_copies[k].wait_recv()
            image_diagonals.append(push(part(ibuf, 1, k), part(ibuf, 3, k), by_low))
        else:
            low_copies[k].wait_recv()
            image_diagonals.append(push(part(ibuf, 2, k), part(ibuf, 3, k), by_x))
        high_copies[k].wait_recv()
        diagonal_copies.append(push(part(tbuf, 2, k), part(tbuf, 3, k), by_y))
        core_copies.append(push(part(tbuf, 2, k), part(tbuf, 6, k), by_core))
    for k in chunks:
        diagonal_copies[k].wait_recv()
        core_copies.append(push(part(tbuf, 3, k), part(tbuf, 7, k), by_core))
    arrived(core_copies)
    for k in chunks:
        (low_copies if k % 2 == 0 else x_copies)[k].wait_recv()
    arrived(image_diagonals)

    scale = scale_ref[0, 0]
    shift = shift_ref[0, 0]
    texts = 8 * share
    group = texts // 3 if texts % 384 == 0 else texts
    for first in range(0, texts, group):
        energy = scale * dot_nt(ibuf[...], tbuf[first : first + group, :]) + shift
        row = lax.broadcasted_iota(jnp.int32, energy.shape, 0)
        column = lax.broadcasted_iota(jnp.int32, energy.shape, 1) + first
        same = jnp.logical_and(row == column, row < share)
        weight = scale * jax.nn.sigmoid(jnp.where(same, -energy, energy))
        weights[:, first : first + group] = jnp.where(same, -weight, weight).astype(BF16)

    d_part[of(2), :] = dot(weights[of(3), :], tbuf[...]).astype(BF16)
    through = [
        push(part(d_part, 2, k), part(d_through, 0, k), by_x if k % 2 == 0 else by_low) for k in chunks
    ]
    d_near[...] = dot(weights[share : 3 * share, :], tbuf[...])
    dir_copies = []
    for k in chunks:
        at = 0 if k % 2 == 0 else 1
        d_part[lines(at, k)] = d_near[lines(at, k)].astype(BF16)
        dir_copies.append(push(part(d_part, at, k), part(d_land, at, k), (by_x, by_low)[at]))

    c_part[...] = dot_tn(weights[:, 4 * share :], ibuf[...]).astype(BF16)
    core_copies = [push(block(c_part, at), block(c_land, at), by_core) for at in (3, 1, 2, 0)]
    s_own[...] = dot_tn(weights[:, : 4 * share], ibuf[...])
    core_copies[0].wait_recv()
    y_part[of(1), :] = (s_own[of(3), :] + c_land[of(3), :].astype(F32)).astype(BF16)
    diagonal_copies = [push(part(y_part, 1, k), part(y_land, 1, k), by_y) for k in chunks]
    core_copies[1].wait_recv()
    y_part[of(0), :] = (s_own[of(1), :] + c_land[of(1), :].astype(F32)).astype(BF16)
    y_copies = [push(part(y_part, 0, k), part(y_land, 0, k), by_y) for k in chunks]
    for k in chunks:
        at = 1 if k % 2 == 0 else 0
        through[k].wait_recv()
        d_part[lines(at, k)] = (d_near[lines(at, k)] + d_through[lines(0, k)].astype(F32)).astype(BF16)
        dir_copies.append(push(part(d_part, at, k), part(d_land, at, k), (by_x, by_low)[at]))
    d_own[...] = dot(weights[of(0), :], tbuf[...])
    arrived(core_copies[2:])
    for at in (0, 2):
        s_own[of(at), :] = s_own[of(at), :] + c_land[of(at), :].astype(F32)
    high_copies = []
    for k in chunks:
        diagonal_copies[k].wait_recv()
        h_part[lines(0, k)] = (s_own[lines(2, k)] + y_land[lines(1, k)].astype(F32)).astype(BF16)
        high_copies.append(push(part(h_part, 0, k), part(h_land, 0, k), by_high))

    arrived(dir_copies)
    for k in chunks:
        total = d_own[lines(0, k)] + d_land[lines(0, k)].astype(F32) + d_land[lines(1, k)].astype(F32)
        g_part[lines(0, k)] = norm_back(total, ibuf[lines(0, k)], inv_image[k]).astype(BF16)
    grad_copy = push(g_part, g_land, by_x)

    gain = gain_ref[...].reshape(1, width)
    mine_first = head == 0
    gains = jnp.where(mine_first, gain[:, :cols], gain[:, cols:])

    def backward(at, upstream):
        grad_b = upstream[...]
        for first, size in tiles:
            span = slice(first, first + size)
            values[of(at), span] = (dot_nt(grad_b, exit_[span, :]) * slope[of(at), span]).astype(BF16)
        total = dot(values[of(at), :], entry[...])
        lower = total[:, :cols]
        upper = total[:, cols:]
        n_part[of(at), :cols] = jnp.where(mine_first, upper, lower).astype(BF16)
        grad_normed = jnp.where(mine_first, lower, upper)
        scaled = total * gain
        one_sum = jnp.sum(scaled, axis=-1, keepdims=True)
        two_sum = jnp.sum(scaled * centred_ref[of(at), :], axis=-1, keepdims=True)
        lane = lax.broadcasted_iota(jnp.int32, (share, n_part.shape[1] - cols), 1)
        packed = jnp.zeros(lane.shape, F32)
        for place, term in enumerate(split_three(one_sum) + split_three(two_sum)):
            packed = jnp.where(lane == place, term.astype(F32), packed)
        n_part[of(at), cols:] = packed.astype(BF16)
        return push(block(n_part, at), block(n_land, 1 - at), by_x), grad_normed, one_sum, two_sum

    def finish(at, upstream, grad_normed, one_sum, two_sum):
        grad_float = upstream[...].astype(F32)
        grad_float = jnp.where(mine_first, grad_float[:, :cols], grad_float[:, cols:])
        centred = centred_ref[of(at), :]
        centred = jnp.where(mine_first, centred[:, :cols], centred[:, cols:])
        grad_normed = grad_normed + n_land[of(at), :cols].astype(F32)
        sums = n_land[of(at), cols:].astype(F32)
        mean_one = (one_sum + (sums[:, 0:1] + sums[:, 1:2] + sums[:, 2:3])) * (1.0 / width)
        mean_two = (two_sum + (sums[:, 3:4] + sums[:, 4:5] + sums[:, 5:6])) * (1.0 / width)
        result = grad_float + inv_std[of(at)] * (grad_normed * gains - mean_one - centred * mean_two)
        out_image[(own_rows, other_rows)[at], :] = result

    text_copies = []

    def text_back(k):
        high_copies[k].wait_recv()
        y_copies[k].wait_recv()
        total = s_own[lines(0, k)] + y_land[lines(0, k)].astype(F32) + h_land[lines(0, k)].astype(F32)
        gt_part[lines(0, k)] = norm_back(total, tbuf[lines(0, k)], inv_text[k]).astype(BF16)
        text_copies.append(push(part(gt_part, 0, k), part(gt_land, 0, k), by_x))

    own_copy, *own_terms = backward(0, g_part)
    text_back(0)
    grad_copy.wait_recv()
    their_copy, *their_terms = backward(1, g_land)
    for k in chunks[1:]:
        text_back(k)
    own_copy.wait_recv()
    finish(1, g_land, *their_terms)
    out_text[own_rows, :] = dot_nt(gt_part[...], mapping[...])
    their_copy.wait_recv()
    finish(0, g_part, *own_terms)
    arrived(text_copies)
    out_text[other_rows, :] = dot_nt(gt_land[...], mapping[...])
    for copy in pending:
        copy.wait_send()


def square_device(pic, cap, gain, entry, exit_, mapping, scale, shift):
    rows, width = pic.shape
    cols = cap.shape[1]
    share = rows // 2
    hidden = entry.shape[1]
    flipped = entry.T
    anywhere = pl.BlockSpec(memory_space=pl.ANY)
    vmem = pl.BlockSpec(memory_space=pltpu.VMEM)
    smem = pl.BlockSpec(memory_space=pltpu.SMEM)
    dma = pltpu.SemaphoreType.DMA

    def blocks(count, dtype=BF16):
        return pltpu.VMEM((count * share, width), dtype)

    loads = 6 + 2 * pl.cdiv(hidden, TILE)
    copies = 64
    extended = 128 * (cols // 128 + 1)
    return pl.pallas_call(
        square_body,
        out_shape=(
            jax.ShapeDtypeStruct((rows, cols), F32),
            jax.ShapeDtypeStruct((rows, mapping.shape[0]), F32),
        ),
        in_specs=[anywhere] * 6 + [smem, smem],
        out_specs=(vmem, vmem),
        scratch_shapes=[
            pltpu.VMEM(pic.shape, BF16),
            pltpu.VMEM(cap.shape, BF16),
            pltpu.VMEM(gain.shape, F32),
            pltpu.VMEM(flipped.shape, BF16),
            pltpu.VMEM(exit_.shape, BF16),
            pltpu.VMEM(mapping.shape, BF16),
            dma((loads,)),
            pltpu.VMEM((rows, width), BF16),
            pltpu.VMEM((rows, width), F32),
            pltpu.VMEM((rows, hidden), BF16),
            pltpu.VMEM((rows, hidden), F32),
            blocks(1, F32),
            blocks(1),
            blocks(1),
            blocks(1, F32),
            blocks(1),
            blocks(1),
            blocks(8),
            blocks(4),
            pltpu.VMEM((4 * share, 8 * share), BF16),
            blocks(1, F32),
            blocks(2, F32),
            blocks(3),
            blocks(1),
            blocks(2),
            blocks(1),
            blocks(1),
            blocks(4, F32),
            blocks(4),
            blocks(4),
            blocks(2),
            blocks(2),
            blocks(1),
            blocks(1),
            blocks(1),
            blocks(1),
            pltpu.VMEM((rows, extended), BF16),
            pltpu.VMEM((rows, extended), BF16),
            dma((copies,)),
            dma((copies,)),
        ],
        compiler_params=pltpu.CompilerParams(
            collective_id=0, has_side_effects=True, vmem_limit_bytes=60 * 2**20
        ),
        name="contrastive_square",
    )(
        pic,
        cap,
        gain,
        flipped,
        exit_,
        mapping,
        scale.reshape(1, 1),
        shift.reshape(1, 1),
    )


def solution(mesh):
    in_specs = (
        P("dp", None),
        P("dp", "mp"),
        P(),
        P(None, "mp"),
        P("mp", None),
        P("mp", None),
        P(),
        P(),
    )
    out_specs = (P("dp", "mp"), P("dp", "mp"))
    square = mesh.shape["mp"] == 2 and mesh.shape["dp"] == 16
    return jax.shard_map(
        square_device if square else per_device, mesh=mesh, in_specs=in_specs, out_specs=out_specs, check_vma=False
    )
```

```python
import functools
import math

import jax
import jax.numpy as jnp
from jax import lax
from jax.experimental import pallas as pl
from jax.experimental.pallas import tpu as pltpu
from jax.sharding import PartitionSpec as P

F32 = jnp.float32
BF16 = jnp.bfloat16
MESH = pl.DeviceIdType.MESH
TILE = 512
ROOT = math.sqrt(2.0 / math.pi)
NT = (((1,), (1,)), ((), ()))
TN = (((0,), (0,)), ((), ()))


def dot(a, b):
    return jnp.dot(a, b, preferred_element_type=F32)


def dot_nt(a, b):
    return lax.dot_general(a, b, NT, preferred_element_type=F32)


def gelu_pair(x):
    square = x * x
    t = jnp.tanh(ROOT * (x + 0.044715 * (square * x)))
    half = 0.5 * (1.0 + t)
    slope = half + 0.5 * x * (1.0 - t * t) * (ROOT * (1.0 + 0.134145 * square))
    return x * half, slope


def norm_back(upstream, unit_rows, inverse):
    unit_float = unit_rows.astype(F32)
    along = jnp.sum(unit_float * upstream, axis=-1, keepdims=True)
    return inverse * (upstream - unit_float * along)


def body(
    n,
    heads,
    pic_hbm,
    cap_hbm,
    gain_ref,
    entry_hbm,
    exit_hbm,
    map_hbm,
    scale_ref,
    shift_ref,
    out_go,
    out_rest,
    out_text,
    pic,
    cap,
    entry,
    exit_,
    mapping,
    load_sem,
    normed,
    values,
    slope,
    weights,
    acc,
    own_f32,
    parts,
    lands,
    fulls,
    ring_text,
    ring_image,
    gains,
    centres,
    norm_own,
    norm_part,
    norm_land,
    sums_part,
    sums_land,
    part_send,
    part_recv,
    full_send,
    full_recv,
    norm_send,
    norm_recv,
    sums_send,
    sums_recv,
    ring_send,
    ring_recv,
):
    rows, width = pic.shape
    share = rows // heads
    hidden = exit_.shape[0]
    cols = width // heads
    me = lax.axis_index("dp")
    head = lax.axis_index("mp")
    length = n // 4

    def place(index):
        z = index // 4
        y = (index // 2) % 2
        return 2 * (z * (1 - y) + (2 * length - 1 - z) * y) + index % 2

    def device(position):
        position = (position + n) % n
        chip = position // 2
        y = chip // length
        z = chip * (1 - y) + (2 * length - 1 - chip) * y
        return (z * 2 + y) * 2 + position % 2

    pos = place(me)
    right = device(pos + 1)
    left = device(pos - 1)
    forward = n // 2
    backward = n - 1 - forward

    loads = []
    for at, (src, dst) in enumerate(
        (
            (cap_hbm, cap),
            (map_hbm, mapping),
            (pic_hbm, pic),
            (entry_hbm, entry),
            (exit_hbm, exit_),
        )
    ):
        copy = pltpu.make_async_copy(src, dst, load_sem.at[at])
        copy.start()
        loads.append(copy)

    barrier = pltpu.get_barrier_semaphore()
    for neighbour in (left, right):
        pl.semaphore_signal(barrier, inc=1, device_id={"dp": neighbour}, device_id_type=MESH)
    for o in range(1, heads):
        pl.semaphore_signal(
            barrier, inc=1, device_id={"mp": (head + o) % heads}, device_id_type=MESH
        )

    def ring_copy(which, buf, way, step):
        block = device(pos - step if way == 0 else pos + step)
        return pltpu.make_async_remote_copy(
            src_ref=buf.at[block],
            dst_ref=buf.at[block],
            send_sem=ring_send.at[which, way, step],
            recv_sem=ring_recv.at[which, way, step],
            device_id={"dp": right if way == 0 else left},
            device_id_type=MESH,
        )

    def ring_start(which, buf, step):
        if step < forward:
            ring_copy(which, buf, 0, step).start()
        if step < backward:
            ring_copy(which, buf, 1, step).start()

    def ring_next(which, buf, step):
        for way, count in ((0, forward), (1, backward)):
            if step < count:
                block = device(pos - step - 1 if way == 0 else pos + step + 1)
                pltpu.make_async_remote_copy(
                    src_ref=buf.at[block],
                    dst_ref=buf.at[block],
                    send_sem=ring_send.at[which, way, step],
                    recv_sem=ring_recv.at[which, way, step],
                    device_id={"dp": right if way == 0 else left},
                    device_id_type=MESH,
                ).wait_recv()
                if step + 1 < count:
                    ring_copy(which, buf, way, step + 1).start()

    def ring_end(which, buf):
        for way, count in ((0, forward), (1, backward)):
            for step in range(count):
                ring_copy(which, buf, way, step).wait_send()

    def exchange(src, dst, send, recv, spread, span=None):
        def part(ref, at):
            return ref.at[at] if span is None else ref.at[at, :, span]

        copies = []
        for o in range(1, heads):
            to = (head + o) % heads
            source = (head + heads - o) % heads
            sent = pltpu.make_async_remote_copy(
                src_ref=part(src, to if spread else head),
                dst_ref=part(dst, head),
                send_sem=send.at[o],
                recv_sem=recv.at[o],
                device_id={"mp": to},
                device_id_type=MESH,
            )
            got = pltpu.make_async_remote_copy(
                src_ref=part(dst, source),
                dst_ref=part(dst, source),
                send_sem=send.at[o],
                recv_sem=recv.at[o],
                device_id={"mp": to},
                device_id_type=MESH,
            )
            copies.append((sent, got))
        for sent, got in copies:
            sent.start()
        return copies

    def arrived(copies):
        for sent, got in copies:
            got.wait_recv()

    def finished(copies):
        for sent, got in copies:
            sent.wait_send()

    def scatter_start(which, product):
        copies = []
        for at, (first, size) in enumerate(pieces):
            columns = pl.ds(first, size)
            total = product(slice(first, first + size))
            for p in range(heads):
                piece = total[p * share : (p + 1) * share]
                own_f32[p, :, first : first + size] = piece
                parts[which, p, :, first : first + size] = piece.astype(BF16)
            copies += exchange(
                parts.at[which],
                lands.at[which],
                part_send.at[which, at],
                part_recv.at[which, at],
                True,
                columns,
            )
        return copies

    def scatter_sum(which, copies, mine):
        arrived(copies)
        for o in range(1, heads):
            mine = mine + lands[which, (head + heads - o) % heads].astype(F32)
        return mine

    def share_start(which, mine):
        fulls[which, head] = mine
        return exchange(
            fulls.at[which], fulls.at[which], full_send.at[which], full_recv.at[which], False
        )

    def full(which):
        return jnp.concatenate([fulls[which, p] for p in range(heads)], axis=0)

    pending = []
    pieces = [(first, min(TILE, width - first)) for first in range(0, width, TILE)]

    loads[0].wait()
    loads[1].wait()
    pl.semaphore_wait(barrier, 2 + heads - 1)
    text_copies = scatter_start(0, lambda span: dot(cap[...], mapping[:, span]))
    pending.append(text_copies)
    text_mine = own_f32[head]

    loads[2].wait()
    image_float = pic[...].astype(F32)
    mean_row = jnp.mean(image_float, axis=-1, keepdims=True)
    variance = jnp.mean((image_float - mean_row) ** 2, axis=-1, keepdims=True)
    inv_std = lax.rsqrt(variance + 1e-06)
    gain = gain_ref[...].reshape(1, width)
    centred = (image_float - mean_row) * inv_std
    normed[...] = (centred * gain).astype(BF16)
    for p in range(heads):
        gains[p] = gain[:, p * cols : (p + 1) * cols]
        centres[p] = centred[:, p * cols : (p + 1) * cols]

    text_out = scatter_sum(0, text_copies, text_mine)
    inv_text = lax.rsqrt(jnp.sum(text_out * text_out, axis=-1, keepdims=True) + 1e-06)
    unit_text = (text_out * inv_text).astype(BF16)
    ring_text[me] = unit_text
    ring_start(0, ring_text, 0)
    text_full = share_start(0, unit_text)
    pending.append(text_full)

    loads[3].wait()
    loads[4].wait()
    tiles = [(first, min(TILE, hidden - first)) for first in range(0, hidden, TILE)]
    text_steps = iter(range(forward))

    def advance(steps, which, buf, count):
        for _ in range(count):
            step = next(steps, None)
            if step is not None:
                ring_next(which, buf, step)

    for at, (first, size) in enumerate(tiles):
        span = slice(first, first + size)
        value, grad = gelu_pair(dot_nt(normed[...], entry[span, :]))
        slope[:, span] = grad
        values[:, span] = value.astype(BF16)
        if at % 2 == 1:
            advance(text_steps, 0, ring_text, 1)
    image_copies = scatter_start(1, lambda span: dot(values[...], exit_[:, span]))
    pending.append(image_copies)
    mine = own_f32[head] + pic[pl.ds(pl.multiple_of(head * share, 8), share), :].astype(F32)
    advance(text_steps, 0, ring_text, 2)
    image_out = scatter_sum(1, image_copies, mine)
    inv_image = lax.rsqrt(jnp.sum(image_out * image_out, axis=-1, keepdims=True) + 1e-06)
    unit_image = (image_out * inv_image).astype(BF16)
    ring_image[me] = unit_image
    image_full = share_start(1, unit_image)
    pending.append(image_full)
    ring_start(1, ring_image, 0)
    advance(text_steps, 0, ring_text, forward)
    ring_end(0, ring_text)
    arrived(image_full)
    arrived(text_full)

    scale = scale_ref[0, 0]
    shift = shift_ref[0, 0]
    group = 4 if share % 16 == 0 else 1

    def weigh(mine, block, g):
        energy = scale * dot_nt(mine, block) + shift
        shape = (rows, group * share)
        column = lax.broadcasted_iota(jnp.int32, shape, 1)
        ident = column + (g * (group * rows) + head * share)
        for j in range(1, group):
            ident = ident + jnp.where(column >= j * share, rows - share, 0)
        same = ident == lax.broadcasted_iota(jnp.int32, shape, 0) + me * rows
        weight = scale * jax.nn.sigmoid(jnp.where(same, -energy, energy))
        return jnp.where(same, -weight, weight).astype(BF16)

    def terms(rows_ref, buf):
        mine = full(rows_ref)
        if group > 1 and (group * share) % 128 == 0:
            for g in range(n // group):
                block = buf[g * group : (g + 1) * group].reshape(group * share, width)
                weights[:, g * group * share : (g + 1) * group * share] = weigh(mine, block, g)
            return lambda span: dot(
                weights[...], buf[:, :, span].reshape(n * share, span.stop - span.start)
            )
        acc[...] = jnp.zeros_like(acc)

        def one(g, carry):
            block = buf[g] if group == 1 else buf[pl.ds(g * group, group)].reshape(group * share, width)
            acc[...] += dot(weigh(full(rows_ref), block, g), block)
            return carry

        lax.fori_loop(0, n // group, one, 0)
        return lambda span: acc[:, span]

    image_steps = iter(range(forward))
    dir_copies = scatter_start(2, terms(1, ring_text))
    pending.append(dir_copies)
    dir_mine = own_f32[head]
    advance(image_steps, 1, ring_image, 4)
    image_dir = scatter_sum(2, dir_copies, dir_mine)
    grad_out = norm_back(image_dir, fulls[1, head], inv_image)
    grad_full = share_start(2, grad_out.astype(BF16))
    pending.append(grad_full)
    advance(image_steps, 1, ring_image, forward)
    ring_end(1, ring_image)

    dirs_copies = scatter_start(3, terms(0, ring_image))
    pending.append(dirs_copies)
    dirs_mine = own_f32[head]

    arrived(grad_full)
    for p in range(heads):
        out_go[p * share : (p + 1) * share] = fulls[2, p]
    grad_b = full(2)
    for at, (first, size) in enumerate(tiles):
        span = slice(first, first + size)
        values[:, span] = (dot_nt(grad_b, exit_[span, :]) * slope[:, span]).astype(BF16)
    total = dot(values[...], entry[...])
    for p in range(heads):
        piece = total[:, p * cols : (p + 1) * cols]
        norm_own[p] = piece
        norm_part[p] = piece.astype(BF16)
    norm_copies = exchange(norm_part, norm_land, norm_send, norm_recv, True)
    scaled = total * gain_ref[...].reshape(1, width)
    one_sum = jnp.sum(scaled, axis=-1, keepdims=True)
    centred = (pic[...].astype(F32) - mean_row) * inv_std
    two_sum = jnp.sum(scaled * centred, axis=-1, keepdims=True)
    lane = lax.broadcasted_iota(jnp.int32, (rows, 128), 1)
    sums_part[head] = jnp.where(lane == 0, one_sum, two_sum)
    sums_copies = exchange(sums_part, sums_land, sums_send, sums_recv, False)
    pending.append(norm_copies)
    pending.append(sums_copies)

    text_dir = scatter_sum(3, dirs_copies, dirs_mine)
    grad_text_out = norm_back(text_dir, fulls[0, head], inv_text).astype(BF16)
    last_full = share_start(3, grad_text_out)
    pending.append(last_full)

    arrived(norm_copies)
    arrived(sums_copies)
    grad_normed = norm_own[head]
    sums = sums_part[head]
    for o in range(1, heads):
        source = (head + heads - o) % heads
        grad_normed = grad_normed + norm_land[source].astype(F32)
        sums = sums + sums_land[source]
    mean_one = sums[:, 0:1] * (1.0 / width)
    mean_two = sums[:, 1:2] * (1.0 / width)
    centred = centres[head]
    scaled = grad_normed * gains[head]
    out_rest[...] = inv_std * (scaled - mean_one - centred * mean_two)

    arrived(last_full)
    out_text[...] = dot_nt(full(3), mapping[...])
    for copies in pending:
        finished(copies)


def per_device(pic, cap, gain, entry, exit_, mapping, scale, shift):
    rows, width = pic.shape
    n = lax.axis_size("dp")
    heads = lax.axis_size("mp")
    cols = cap.shape[1]
    share = rows // heads
    hidden = entry.shape[1]
    flipped = entry.T
    anywhere = pl.BlockSpec(memory_space=pl.ANY)
    vmem = pl.BlockSpec(memory_space=pltpu.VMEM)
    smem = pl.BlockSpec(memory_space=pltpu.SMEM)
    dma = pltpu.SemaphoreType.DMA
    go, rest, text = pl.pallas_call(
        functools.partial(body, n, heads),
        out_shape=(
            jax.ShapeDtypeStruct((rows, width), BF16),
            jax.ShapeDtypeStruct((rows, cols), F32),
            jax.ShapeDtypeStruct((rows, mapping.shape[0]), F32),
        ),
        in_specs=[anywhere, anywhere, vmem, anywhere, anywhere, anywhere, smem, smem],
        out_specs=(vmem, vmem, vmem),
        scratch_shapes=[
            pltpu.VMEM(pic.shape, BF16),
            pltpu.VMEM(cap.shape, BF16),
            pltpu.VMEM(flipped.shape, BF16),
            pltpu.VMEM(exit_.shape, BF16),
            pltpu.VMEM(mapping.shape, BF16),
            dma((5,)),
            pltpu.VMEM((rows, width), BF16),
            pltpu.VMEM((rows, hidden), BF16),
            pltpu.VMEM((rows, hidden), F32),
            pltpu.VMEM((rows, n * share), BF16),
            pltpu.VMEM((rows, width), F32),
            pltpu.VMEM((heads, share, width), F32),
            pltpu.VMEM((4, heads, share, width), BF16),
            pltpu.VMEM((4, heads, share, width), BF16),
            pltpu.VMEM((4, heads, share, width), BF16),
            pltpu.VMEM((n, share, width), BF16),
            pltpu.VMEM((n, share, width), BF16),
            pltpu.VMEM((heads, 1, cols), F32),
            pltpu.VMEM((heads, rows, cols), F32),
            pltpu.VMEM((heads, rows, cols), F32),
            pltpu.VMEM((heads, rows, cols), BF16),
            pltpu.VMEM((heads, rows, cols), BF16),
            pltpu.VMEM((heads, rows, 128), F32),
            pltpu.VMEM((heads, rows, 128), F32),
            dma((4, pl.cdiv(width, TILE), heads)),
            dma((4, pl.cdiv(width, TILE), heads)),
            dma((4, heads)),
            dma((4, heads)),
            dma((heads,)),
            dma((heads,)),
            dma((heads,)),
            dma((heads,)),
            dma((2, 2, n // 2)),
            dma((2, 2, n // 2)),
        ],
        compiler_params=pltpu.CompilerParams(
            collective_id=0, has_side_effects=True, vmem_limit_bytes=60 * 2**20
        ),
        name="contrastive",
    )(
        pic,
        cap,
        gain,
        flipped,
        exit_,
        mapping,
        scale.reshape(1, 1),
        shift.reshape(1, 1),
    )
    first = lax.axis_index("mp") * cols
    grad_image = lax.dynamic_slice_in_dim(go, first, cols, 1).astype(F32) + rest
    return grad_image, text


def flipped_bit(index, bit):
    return index + bit * (1 - 2 * ((index // bit) % 2))


def dot_tn(a, b):
    return lax.dot_general(a, b, TN, preferred_element_type=F32)


def split_three(x):
    high = x.astype(BF16)
    rest = x - high.astype(F32)
    middle = rest.astype(BF16)
    return high, middle, (rest - middle.astype(F32)).astype(BF16)


def square_body(
    pic_hbm,
    cap_hbm,
    gain_hbm,
    entry_hbm,
    exit_hbm,
    map_hbm,
    scale_hbm,
    shift_hbm,
    out_image_hbm,
    out_text_hbm,
    scale_ref,
    shift_ref,
    out_image,
    out_text,
    store_sem,
    pic,
    cap,
    gain_ref,
    entry,
    exit_,
    mapping,
    load_sem,
    normed,
    centred_ref,
    values,
    slope,
    t_own,
    t_part,
    t_land,
    i_own,
    i_part,
    i_land,
    tbuf,
    ibuf,
    weights,
    d_own,
    d_near,
    d_part,
    d_through,
    d_land,
    g_part,
    g_land,
    s_own,
    c_part,
    c_land,
    y_part,
    y_land,
    h_part,
    h_land,
    gt_part,
    gt_land,
    n_part,
    n_land,
    send_sem,
    recv_sem,
):
    rows, width = pic.shape
    share = rows // 2
    hidden = exit_.shape[0]
    cols = width // 2
    me = lax.axis_index("dp")
    head = lax.axis_index("mp")
    other = 1 - head
    by_core = {"dp": flipped_bit(me, 1)}
    by_y = {"dp": flipped_bit(me, 2)}
    by_low = {"dp": flipped_bit(me, 4)}
    by_high = {"dp": flipped_bit(me, 8)}
    by_x = {"mp": other}
    own_rows = pl.ds(pl.multiple_of(head * share, 16), share)
    other_rows = pl.ds(pl.multiple_of(other * share, 16), share)
    tiles = [(first, min(TILE, hidden - first)) for first in range(0, hidden, TILE)]
    chunk = share // 3 if share % 48 == 0 else share
    chunks = range(share // chunk)
    spans = [slice(first, min(first + TILE, width)) for first in range(0, width, TILE)]
    x_first = [k == 2 for k in chunks]

    def block(ref, at):
        return ref.at[pl.ds(at * share, share)]

    def part(ref, at, k):
        return ref.at[pl.ds(at * share + k * chunk, chunk)]

    def of(at):
        return slice(at * share, (at + 1) * share)

    def lines(at, k):
        return slice(at * share + k * chunk, at * share + (k + 1) * chunk)

    load_count = 0

    def load(src, dst):
        nonlocal load_count
        copy = pltpu.make_async_copy(src, dst, load_sem.at[load_count])
        load_count += 1
        copy.start()
        return copy

    cap_loads = [
        load(cap_hbm.at[other_rows], block(cap, 1)),
        load(map_hbm, mapping),
        load(cap_hbm.at[own_rows], block(cap, 0)),
    ]
    pic_loads = [
        load(pic_hbm.at[own_rows], block(pic, 0)),
        load(pic_hbm.at[other_rows], block(pic, 1)),
        load(gain_hbm, gain_ref),
        load(scale_hbm, scale_ref),
        load(shift_hbm, shift_ref),
    ]
    entry_loads = [
        load(entry_hbm.at[pl.ds(first, size)], entry.at[pl.ds(first, size)]) for first, size in tiles
    ]

    barrier = pltpu.get_barrier_semaphore()
    partners = (by_x, by_y, by_high, by_low, by_core)
    for partner in partners:
        pl.semaphore_signal(barrier, inc=1, device_id=partner, device_id_type=MESH)

    pending = []

    def push(src, dst, partner):
        at = len(pending)
        copy = pltpu.make_async_remote_copy(
            src_ref=src,
            dst_ref=dst,
            send_sem=send_sem.at[at],
            recv_sem=recv_sem.at[at],
            device_id=partner,
            device_id_type=MESH,
        )
        copy.start()
        pending.append(copy)
        return copy

    def arrived(copies):
        for copy in copies:
            copy.wait_recv()

    for copy in cap_loads:
        copy.wait()
    t_part[...] = dot(cap[share:], mapping[...]).astype(BF16)
    pl.semaphore_wait(barrier, len(partners))
    text_partials = [push(part(t_part, 0, k), part(t_land, 0, k), by_x) for k in chunks]
    t_own[...] = dot(cap[:share], mapping[...])
    exit_loads = [
        load(exit_hbm.at[pl.ds(first, size)], exit_.at[pl.ds(first, size)]) for first, size in tiles
    ]

    for copy in pic_loads:
        copy.wait()
    image_float = pic[...].astype(F32)
    mean_row = jnp.mean(image_float, axis=-1, keepdims=True)
    variance = jnp.mean((image_float - mean_row) ** 2, axis=-1, keepdims=True)
    inv_std = lax.rsqrt(variance + 1e-06)
    gain = gain_ref[...].reshape(1, width)
    centred = (image_float - mean_row) * inv_std
    centred_ref[...] = centred
    normed[...] = (centred * gain).astype(BF16)

    def unit_rows(own, land, k, dst):
        total = own[lines(0, k)] + land[lines(0, k)].astype(F32)
        inverse = lax.rsqrt(jnp.sum(total * total, axis=-1, keepdims=True) + 1e-06)
        dst[lines(0, k)] = (total * inverse).astype(BF16)
        return inverse

    inv_text = []
    high_copies = []
    y_copies = []
    early_copies = []
    late_copies = []

    def send_high(k):
        high_copies.append(push(part(tbuf, 0, k), part(tbuf, 4, k), by_high))

    def text_chunk(k):
        text_partials[k].wait_recv()
        inv_text.append(unit_rows(t_own, t_land, k, tbuf))
        if k < 2:
            send_high(k)
        y_copies.append(push(part(tbuf, 0, k), part(tbuf, 1, k), by_y))
        early_copies.append(push(part(tbuf, 0, k), part(tbuf, 2, k), by_core))

    for at, ((first, size), copy) in enumerate(zip(tiles, entry_loads)):
        copy.wait()
        span = slice(first, first + size)
        value, grad = gelu_pair(dot_nt(normed[...], entry[span, :]))
        slope[:, span] = grad
        values[:, span] = value.astype(BF16)
        if at == len(tiles) - 2:
            text_chunk(0)
    for copy in exit_loads:
        copy.wait()
    for span in spans:
        i_part[:, span] = dot(values[share:], exit_[:, span]).astype(BF16)
    image_partials = [push(part(i_part, 0, k), part(i_land, 0, k), by_x) for k in chunks]
    for k in chunks[1:]:
        text_chunk(k)
    for span in spans:
        i_own[:, span] = dot(values[:share], exit_[:, span]) + pic[:share, span].astype(F32)

    inv_image = []
    x_copies = []
    low_copies = []
    for k in chunks:
        image_partials[k].wait_recv()
        inv_image.append(unit_rows(i_own, i_land, k, ibuf))
        x_copies.append(push(part(ibuf, 0, k), part(ibuf, 1, k), by_x))
        low_copies.append(push(part(ibuf, 0, k), part(ibuf, 2, k), by_low))
        if k == 2:
            send_high(2)

    for k in chunks:
        y_copies[k].wait_recv()
        early_copies.append(push(part(tbuf, 1, k), part(tbuf, 3, k), by_core))
    diagonal_copies = []
    image_copies = []
    for k in chunks:
        if x_first[k]:
            x_copies[k].wait_recv()
            image_copies.append(push(part(ibuf, 1, k), part(ibuf, 3, k), by_low))
        else:
            low_copies[k].wait_recv()
            image_copies.append(push(part(ibuf, 2, k), part(ibuf, 3, k), by_x))
        high_copies[k].wait_recv()
        diagonal_copies.append(push(part(tbuf, 4, k), part(tbuf, 5, k), by_y))
        late_copies.append(push(part(tbuf, 4, k), part(tbuf, 6, k), by_core))
    for k in chunks:
        (low_copies if x_first[k] else x_copies)[k].wait_recv()
    arrived(image_copies)
    arrived(early_copies)

    scale = scale_ref[0, 0]
    shift = shift_ref[0, 0]
    early = slice(0, 4 * share)
    late = slice(4 * share, 8 * share)

    def weigh(texts, paired):
        energy = scale * dot_nt(ibuf[...], tbuf[texts, :]) + shift
        if paired:
            row = lax.broadcasted_iota(jnp.int32, energy.shape, 0)
            column = lax.broadcasted_iota(jnp.int32, energy.shape, 1)
            same = jnp.logical_and(row == column, row < share)
            weight = scale * jax.nn.sigmoid(jnp.where(same, -energy, energy))
            weight = jnp.where(same, -weight, weight)
        else:
            weight = scale * jax.nn.sigmoid(energy)
        weights[:, texts] = weight.astype(BF16)

    weigh(early, True)
    c_part[: 2 * share] = dot_tn(weights[:, 2 * share : 4 * share], ibuf[...]).astype(BF16)
    core_early = push(c_part.at[pl.ds(0, 2 * share)], c_land.at[pl.ds(0, 2 * share)], by_core)
    s_own[: 2 * share] = dot_tn(weights[:, : 2 * share], ibuf[...])
    d_near[...] = dot(weights[:, early], tbuf[early, :])

    for k in chunks:
        diagonal_copies[k].wait_recv()
        late_copies.append(push(part(tbuf, 5, k), part(tbuf, 7, k), by_core))
    core_early.wait_recv()
    y_part[of(0), :] = (s_own[of(1), :] + c_land[of(1), :].astype(F32)).astype(BF16)
    s_own[of(0), :] = s_own[of(0), :] + c_land[of(0), :].astype(F32)
    arrived(late_copies)

    weigh(late, False)

    d_part[of(2), :] = (d_near[of(3), :] + dot(weights[of(3), late], tbuf[late, :])).astype(BF16)
    through = [
        push(part(d_part, 2, k), part(d_through, 0, k), by_x if x_first[k] else by_low) for k in chunks
    ]
    d_near[share : 3 * share] += dot(weights[share : 3 * share, late], tbuf[late, :])
    from_x = [None for k in chunks]
    from_low = [None for k in chunks]

    def send_dir(at, k):
        copy = push(part(d_part, at, k), part(d_land, at, k), (by_x, by_low)[at])
        (from_x, from_low)[at][k] = copy

    for k in chunks:
        at = 0 if x_first[k] else 1
        d_part[lines(at, k)] = d_near[lines(at + 1, k)].astype(BF16)
        send_dir(at, k)

    c_part[2 * share :] = dot_tn(weights[:, 6 * share :], ibuf[...]).astype(BF16)
    core_late = [push(block(c_part, at), block(c_land, at), by_core) for at in (3, 2)]
    s_own[2 * share :] = dot_tn(weights[:, 4 * share : 6 * share], ibuf[...])
    core_late[0].wait_recv()
    y_part[of(1), :] = (s_own[of(3), :] + c_land[of(3), :].astype(F32)).astype(BF16)
    diagonal_copies = [push(part(y_part, 1, k), part(y_land, 1, k), by_y) for k in chunks]
    y_copies = [push(part(y_part, 0, k), part(y_land, 0, k), by_y) for k in chunks]
    for k in chunks:
        at = 1 if x_first[k] else 0
        through[k].wait_recv()
        total = d_near[lines(at + 1, k)] + d_through[lines(0, k)].astype(F32)
        d_part[lines(at, k)] = total.astype(BF16)
        send_dir(at, k)
    d_own[...] = d_near[of(0), :] + dot(weights[of(0), late], tbuf[late, :])
    core_late[1].wait_recv()
    s_own[of(2), :] = s_own[of(2), :] + c_land[of(2), :].astype(F32)
    high_copies = []
    for k in chunks:
        diagonal_copies[k].wait_recv()
        h_part[lines(0, k)] = (s_own[lines(2, k)] + y_land[lines(1, k)].astype(F32)).astype(BF16)
        high_copies.append(push(part(h_part, 0, k), part(h_land, 0, k), by_high))

    grad_copies = []
    for k in chunks:
        from_x[k].wait_recv()
        from_low[k].wait_recv()
        total = d_own[lines(0, k)] + d_land[lines(0, k)].astype(F32) + d_land[lines(1, k)].astype(F32)
        g_part[lines(0, k)] = norm_back(total, ibuf[lines(0, k)], inv_image[k]).astype(BF16)
        grad_copies.append(push(part(g_part, 0, k), part(g_land, 0, k), by_x))

    gain = gain_ref[...].reshape(1, width)
    mine_first = head == 0
    gains = jnp.where(mine_first, gain[:, :cols], gain[:, cols:])
    stores = []

    def store(src, dst, first, begin, count):
        start = pl.multiple_of(begin, 16)
        copy = pltpu.make_async_copy(
            src.at[pl.ds(first, count)], dst.at[pl.ds(start, count)], store_sem.at[len(stores)]
        )
        copy.start()
        stores.append(copy)

    def backward_exit(at, upstream):
        grad_b = upstream[...]
        for begin, size in tiles:
            span = slice(begin, begin + size)
            values[of(at), span] = (dot_nt(grad_b, exit_[span, :]) * slope[of(at), span]).astype(BF16)

    def backward_entry(at):
        total = dot(values[of(at), :], entry[...])
        lower = total[:, :cols]
        upper = total[:, cols:]
        n_part[of(at), :cols] = jnp.where(mine_first, upper, lower).astype(BF16)
        grad_normed = jnp.where(mine_first, lower, upper)
        scaled = total * gain
        one_sum = jnp.sum(scaled, axis=-1, keepdims=True)
        two_sum = jnp.sum(scaled * centred_ref[of(at), :], axis=-1, keepdims=True)
        lane = lax.broadcasted_iota(jnp.int32, (share, n_part.shape[1] - cols), 1)
        packed = jnp.zeros(lane.shape, F32)
        for place, term in enumerate(split_three(one_sum) + split_three(two_sum)):
            packed = jnp.where(lane == place, term.astype(F32), packed)
        n_part[of(at), cols:] = packed.astype(BF16)
        return push(block(n_part, at), block(n_land, 1 - at), by_x), (grad_normed, one_sum, two_sum)

    def finish(at, upstream, grad_normed, one_sum, two_sum):
        lines = of(at)
        grad_float = upstream[...].astype(F32)
        grad_float = jnp.where(mine_first, grad_float[:, :cols], grad_float[:, cols:])
        centred = centred_ref[lines, :]
        centred = jnp.where(mine_first, centred[:, :cols], centred[:, cols:])
        grad_normed = grad_normed + n_land[lines, :cols].astype(F32)
        sums = n_land[lines, cols:].astype(F32)
        mean_one = (one_sum + (sums[:, 0:1] + sums[:, 1:2] + sums[:, 2:3])) * (1.0 / width)
        mean_two = (two_sum + (sums[:, 3:4] + sums[:, 4:5] + sums[:, 5:6])) * (1.0 / width)
        result = grad_float + inv_std[lines] * (grad_normed * gains - mean_one - centred * mean_two)
        out_image[lines, :] = result
        store(out_image, out_image_hbm, at * share, (head, other)[at] * share, share)

    text_copies = []

    def text_back(k):
        high_copies[k].wait_recv()
        y_copies[k].wait_recv()
        total = s_own[lines(0, k)] + y_land[lines(0, k)].astype(F32) + h_land[lines(0, k)].astype(F32)
        gt_part[lines(0, k)] = norm_back(total, tbuf[lines(0, k)], inv_text[k]).astype(BF16)
        text_copies.append(push(part(gt_part, 0, k), part(gt_land, 0, k), by_x))

    backward_exit(0, g_part)
    own_copy, own_terms = backward_entry(0)
    arrived(grad_copies)
    backward_exit(1, g_land)
    text_back(0)
    their_copy, their_terms = backward_entry(1)
    for k in chunks[1:]:
        text_back(k)
    own_copy.wait_recv()
    finish(1, g_land, *their_terms)
    out_text[:share, :] = dot_nt(gt_part[...], mapping[...])
    store(out_text, out_text_hbm, 0, head * share, share)
    their_copy.wait_recv()
    finish(0, g_part, *own_terms)
    arrived(text_copies)
    out_text[share:, :] = dot_nt(gt_land[...], mapping[...])
    store(out_text, out_text_hbm, share, other * share, share)
    for copy in pending:
        copy.wait_send()
    for copy in stores:
        copy.wait()


def hand_over(image_hbm, text_hbm, out_image, out_text, image, text, in_sem, out_sem):
    rows = image.shape[0]
    count = 4 if rows % 32 == 0 else 1
    size = rows // count
    pieces = [
        (src, mid, dst, pl.ds(at * size, size))
        for at in range(count)
        for src, mid, dst in ((image_hbm, image, out_image), (text_hbm, text, out_text))
    ]
    ins = []
    outs = []
    for at, (src, mid, dst, lines) in enumerate(pieces):
        ins.append(pltpu.make_async_copy(src.at[lines], mid.at[lines], in_sem.at[at]))
        outs.append(pltpu.make_async_copy(mid.at[lines], dst.at[lines], out_sem.at[at]))
        ins[at].start()
    for taken, given in zip(ins, outs):
        taken.wait()
        given.start()
    for given in outs:
        given.wait()


def square_device(pic, cap, gain, entry, exit_, mapping, scale, shift):
    rows, width = pic.shape
    cols = cap.shape[1]
    share = rows // 2
    hidden = entry.shape[1]
    flipped = entry.T
    anywhere = pl.BlockSpec(memory_space=pl.ANY)
    dma = pltpu.SemaphoreType.DMA

    def blocks(count, dtype=BF16):
        return pltpu.VMEM((count * share, width), dtype)

    loads = 8 + 2 * pl.cdiv(hidden, TILE)
    copies = 66
    extended = 128 * (cols // 128 + 1)
    results = (
        jax.ShapeDtypeStruct((rows, cols), F32),
        jax.ShapeDtypeStruct((rows, mapping.shape[0]), F32),
    )
    image, text = pl.pallas_call(
        square_body,
        out_shape=results,
        in_specs=[anywhere] * 8,
        out_specs=(anywhere, anywhere),
        scratch_shapes=[
            pltpu.SMEM((1, 1), F32),
            pltpu.SMEM((1, 1), F32),
            pltpu.VMEM((rows, cols), F32),
            pltpu.VMEM((rows, mapping.shape[0]), F32),
            dma((4,)),
            pltpu.VMEM(pic.shape, BF16),
            pltpu.VMEM(cap.shape, BF16),
            pltpu.VMEM(gain.shape, F32),
            pltpu.VMEM(flipped.shape, BF16),
            pltpu.VMEM(exit_.shape, BF16),
            pltpu.VMEM(mapping.shape, BF16),
            dma((loads,)),
            pltpu.VMEM((rows, width), BF16),
            pltpu.VMEM((rows, width), F32),
            pltpu.VMEM((rows, hidden), BF16),
            pltpu.VMEM((rows, hidden), F32),
            blocks(1, F32),
            blocks(1),
            blocks(1),
            blocks(1, F32),
            blocks(1),
            blocks(1),
            blocks(8),
            blocks(4),
            pltpu.VMEM((4 * share, 8 * share), BF16),
            blocks(1, F32),
            blocks(4, F32),
            blocks(3),
            blocks(1),
            blocks(2),
            blocks(1),
            blocks(1),
            blocks(4, F32),
            blocks(4),
            blocks(4),
            blocks(2),
            blocks(2),
            blocks(1),
            blocks(1),
            blocks(1),
            blocks(1),
            pltpu.VMEM((rows, extended), BF16),
            pltpu.VMEM((rows, extended), BF16),
            dma((copies,)),
            dma((copies,)),
        ],
        compiler_params=pltpu.CompilerParams(
            collective_id=0, has_side_effects=True, vmem_limit_bytes=60 * 2**20
        ),
        name="contrastive_square",
    )(
        pic,
        cap,
        gain,
        flipped,
        exit_,
        mapping,
        scale.reshape(1, 1),
        shift.reshape(1, 1),
    )
    return pl.pallas_call(
        hand_over,
        out_shape=results,
        in_specs=[anywhere, anywhere],
        out_specs=(anywhere, anywhere),
        scratch_shapes=[pltpu.VMEM(r.shape, F32) for r in results] + [dma((8,)), dma((8,))],
        compiler_params=pltpu.CompilerParams(vmem_limit_bytes=60 * 2**20),
        name="hand_over",
    )(image, text)


def solution(mesh):
    in_specs = (
        P("dp", None),
        P("dp", "mp"),
        P(),
        P(None, "mp"),
        P("mp", None),
        P("mp", None),
        P(),
        P(),
    )
    out_specs = (P("dp", "mp"), P("dp", "mp"))
    square = mesh.shape["mp"] == 2 and mesh.shape["dp"] == 16
    return jax.shard_map(
        square_device if square else per_device, mesh=mesh, in_specs=in_specs, out_specs=out_specs, check_vma=False
    )
```

```python
import functools
import math

import jax
import jax.numpy as jnp
from jax import lax
from jax.experimental import pallas as pl
from jax.experimental.pallas import tpu as pltpu
from jax.sharding import PartitionSpec as P

F32 = jnp.float32
BF16 = jnp.bfloat16
MESH = pl.DeviceIdType.MESH
TILE = 512
ROOT = math.sqrt(2.0 / math.pi)
NT = (((1,), (1,)), ((), ()))
TN = (((0,), (0,)), ((), ()))


def dot(a, b):
    return jnp.dot(a, b, preferred_element_type=F32)


def dot_nt(a, b):
    return lax.dot_general(a, b, NT, preferred_element_type=F32)


def gelu_pair(x):
    square = x * x
    t = jnp.tanh(ROOT * (x + 0.044715 * (square * x)))
    half = 0.5 * (1.0 + t)
    slope = half + 0.5 * x * (1.0 - t * t) * (ROOT * (1.0 + 0.134145 * square))
    return x * half, slope


def norm_back(upstream, unit_rows, inverse):
    unit_float = unit_rows.astype(F32)
    along = jnp.sum(unit_float * upstream, axis=-1, keepdims=True)
    return inverse * (upstream - unit_float * along)


def body(
    n,
    heads,
    pic_hbm,
    cap_hbm,
    gain_ref,
    entry_hbm,
    exit_hbm,
    map_hbm,
    scale_ref,
    shift_ref,
    out_go,
    out_rest,
    out_text,
    pic,
    cap,
    entry,
    exit_,
    mapping,
    load_sem,
    normed,
    values,
    slope,
    weights,
    acc,
    own_f32,
    parts,
    lands,
    fulls,
    ring_text,
    ring_image,
    gains,
    centres,
    norm_own,
    norm_part,
    norm_land,
    sums_part,
    sums_land,
    part_send,
    part_recv,
    full_send,
    full_recv,
    norm_send,
    norm_recv,
    sums_send,
    sums_recv,
    ring_send,
    ring_recv,
):
    rows, width = pic.shape
    share = rows // heads
    hidden = exit_.shape[0]
    cols = width // heads
    me = lax.axis_index("dp")
    head = lax.axis_index("mp")
    length = n // 4

    def place(index):
        z = index // 4
        y = (index // 2) % 2
        return 2 * (z * (1 - y) + (2 * length - 1 - z) * y) + index % 2

    def device(position):
        position = (position + n) % n
        chip = position // 2
        y = chip // length
        z = chip * (1 - y) + (2 * length - 1 - chip) * y
        return (z * 2 + y) * 2 + position % 2

    pos = place(me)
    right = device(pos + 1)
    left = device(pos - 1)
    forward = n // 2
    backward = n - 1 - forward

    loads = []
    for at, (src, dst) in enumerate(
        (
            (cap_hbm, cap),
            (map_hbm, mapping),
            (pic_hbm, pic),
            (entry_hbm, entry),
            (exit_hbm, exit_),
        )
    ):
        copy = pltpu.make_async_copy(src, dst, load_sem.at[at])
        copy.start()
        loads.append(copy)

    barrier = pltpu.get_barrier_semaphore()
    for neighbour in (left, right):
        pl.semaphore_signal(barrier, inc=1, device_id={"dp": neighbour}, device_id_type=MESH)
    for o in range(1, heads):
        pl.semaphore_signal(
            barrier, inc=1, device_id={"mp": (head + o) % heads}, device_id_type=MESH
        )

    def ring_copy(which, buf, way, step):
        block = device(pos - step if way == 0 else pos + step)
        return pltpu.make_async_remote_copy(
            src_ref=buf.at[block],
            dst_ref=buf.at[block],
            send_sem=ring_send.at[which, way, step],
            recv_sem=ring_recv.at[which, way, step],
            device_id={"dp": right if way == 0 else left},
            device_id_type=MESH,
        )

    def ring_start(which, buf, step):
        if step < forward:
            ring_copy(which, buf, 0, step).start()
        if step < backward:
            ring_copy(which, buf, 1, step).start()

    def ring_next(which, buf, step):
        for way, count in ((0, forward), (1, backward)):
            if step < count:
                block = device(pos - step - 1 if way == 0 else pos + step + 1)
                pltpu.make_async_remote_copy(
                    src_ref=buf.at[block],
                    dst_ref=buf.at[block],
                    send_sem=ring_send.at[which, way, step],
                    recv_sem=ring_recv.at[which, way, step],
                    device_id={"dp": right if way == 0 else left},
                    device_id_type=MESH,
                ).wait_recv()
                if step + 1 < count:
                    ring_copy(which, buf, way, step + 1).start()

    def ring_end(which, buf):
        for way, count in ((0, forward), (1, backward)):
            for step in range(count):
                ring_copy(which, buf, way, step).wait_send()

    def exchange(src, dst, send, recv, spread, span=None):
        def part(ref, at):
            return ref.at[at] if span is None else ref.at[at, :, span]

        copies = []
        for o in range(1, heads):
            to = (head + o) % heads
            source = (head + heads - o) % heads
            sent = pltpu.make_async_remote_copy(
                src_ref=part(src, to if spread else head),
                dst_ref=part(dst, head),
                send_sem=send.at[o],
                recv_sem=recv.at[o],
                device_id={"mp": to},
                device_id_type=MESH,
            )
            got = pltpu.make_async_remote_copy(
                src_ref=part(dst, source),
                dst_ref=part(dst, source),
                send_sem=send.at[o],
                recv_sem=recv.at[o],
                device_id={"mp": to},
                device_id_type=MESH,
            )
            copies.append((sent, got))
        for sent, got in copies:
            sent.start()
        return copies

    def arrived(copies):
        for sent, got in copies:
            got.wait_recv()

    def finished(copies):
        for sent, got in copies:
            sent.wait_send()

    def scatter_start(which, product):
        copies = []
        for at, (first, size) in enumerate(pieces):
            columns = pl.ds(first, size)
            total = product(slice(first, first + size))
            for p in range(heads):
                piece = total[p * share : (p + 1) * share]
                own_f32[p, :, first : first + size] = piece
                parts[which, p, :, first : first + size] = piece.astype(BF16)
            copies += exchange(
                parts.at[which],
                lands.at[which],
                part_send.at[which, at],
                part_recv.at[which, at],
                True,
                columns,
            )
        return copies

    def scatter_sum(which, copies, mine):
        arrived(copies)
        for o in range(1, heads):
            mine = mine + lands[which, (head + heads - o) % heads].astype(F32)
        return mine

    def share_start(which, mine):
        fulls[which, head] = mine
        return exchange(
            fulls.at[which], fulls.at[which], full_send.at[which], full_recv.at[which], False
        )

    def full(which):
        return jnp.concatenate([fulls[which, p] for p in range(heads)], axis=0)

    pending = []
    pieces = [(first, min(TILE, width - first)) for first in range(0, width, TILE)]

    loads[0].wait()
    loads[1].wait()
    pl.semaphore_wait(barrier, 2 + heads - 1)
    text_copies = scatter_start(0, lambda span: dot(cap[...], mapping[:, span]))
    pending.append(text_copies)
    text_mine = own_f32[head]

    loads[2].wait()
    image_float = pic[...].astype(F32)
    mean_row = jnp.mean(image_float, axis=-1, keepdims=True)
    variance = jnp.mean((image_float - mean_row) ** 2, axis=-1, keepdims=True)
    inv_std = lax.rsqrt(variance + 1e-06)
    gain = gain_ref[...].reshape(1, width)
    centred = (image_float - mean_row) * inv_std
    normed[...] = (centred * gain).astype(BF16)
    for p in range(heads):
        gains[p] = gain[:, p * cols : (p + 1) * cols]
        centres[p] = centred[:, p * cols : (p + 1) * cols]

    text_out = scatter_sum(0, text_copies, text_mine)
    inv_text = lax.rsqrt(jnp.sum(text_out * text_out, axis=-1, keepdims=True) + 1e-06)
    unit_text = (text_out * inv_text).astype(BF16)
    ring_text[me] = unit_text
    ring_start(0, ring_text, 0)
    text_full = share_start(0, unit_text)
    pending.append(text_full)

    loads[3].wait()
    loads[4].wait()
    tiles = [(first, min(TILE, hidden - first)) for first in range(0, hidden, TILE)]
    text_steps = iter(range(forward))

    def advance(steps, which, buf, count):
        for _ in range(count):
            step = next(steps, None)
            if step is not None:
                ring_next(which, buf, step)

    for at, (first, size) in enumerate(tiles):
        span = slice(first, first + size)
        value, grad = gelu_pair(dot_nt(normed[...], entry[span, :]))
        slope[:, span] = grad
        values[:, span] = value.astype(BF16)
        if at % 2 == 1:
            advance(text_steps, 0, ring_text, 1)
    image_copies = scatter_start(1, lambda span: dot(values[...], exit_[:, span]))
    pending.append(image_copies)
    mine = own_f32[head] + pic[pl.ds(pl.multiple_of(head * share, 8), share), :].astype(F32)
    advance(text_steps, 0, ring_text, 2)
    image_out = scatter_sum(1, image_copies, mine)
    inv_image = lax.rsqrt(jnp.sum(image_out * image_out, axis=-1, keepdims=True) + 1e-06)
    unit_image = (image_out * inv_image).astype(BF16)
    ring_image[me] = unit_image
    image_full = share_start(1, unit_image)
    pending.append(image_full)
    ring_start(1, ring_image, 0)
    advance(text_steps, 0, ring_text, forward)
    ring_end(0, ring_text)
    arrived(image_full)
    arrived(text_full)

    scale = scale_ref[0, 0]
    shift = shift_ref[0, 0]
    group = 4 if share % 16 == 0 else 1

    def weigh(mine, block, g):
        energy = scale * dot_nt(mine, block) + shift
        shape = (rows, group * share)
        column = lax.broadcasted_iota(jnp.int32, shape, 1)
        ident = column + (g * (group * rows) + head * share)
        for j in range(1, group):
            ident = ident + jnp.where(column >= j * share, rows - share, 0)
        same = ident == lax.broadcasted_iota(jnp.int32, shape, 0) + me * rows
        weight = scale * jax.nn.sigmoid(jnp.where(same, -energy, energy))
        return jnp.where(same, -weight, weight).astype(BF16)

    def terms(rows_ref, buf):
        mine = full(rows_ref)
        if group > 1 and (group * share) % 128 == 0:
            for g in range(n // group):
                block = buf[g * group : (g + 1) * group].reshape(group * share, width)
                weights[:, g * group * share : (g + 1) * group * share] = weigh(mine, block, g)
            return lambda span: dot(
                weights[...], buf[:, :, span].reshape(n * share, span.stop - span.start)
            )
        acc[...] = jnp.zeros_like(acc)

        def one(g, carry):
            block = buf[g] if group == 1 else buf[pl.ds(g * group, group)].reshape(group * share, width)
            acc[...] += dot(weigh(full(rows_ref), block, g), block)
            return carry

        lax.fori_loop(0, n // group, one, 0)
        return lambda span: acc[:, span]

    image_steps = iter(range(forward))
    dir_copies = scatter_start(2, terms(1, ring_text))
    pending.append(dir_copies)
    dir_mine = own_f32[head]
    advance(image_steps, 1, ring_image, 4)
    image_dir = scatter_sum(2, dir_copies, dir_mine)
    grad_out = norm_back(image_dir, fulls[1, head], inv_image)
    grad_full = share_start(2, grad_out.astype(BF16))
    pending.append(grad_full)
    advance(image_steps, 1, ring_image, forward)
    ring_end(1, ring_image)

    dirs_copies = scatter_start(3, terms(0, ring_image))
    pending.append(dirs_copies)
    dirs_mine = own_f32[head]

    arrived(grad_full)
    for p in range(heads):
        out_go[p * share : (p + 1) * share] = fulls[2, p]
    grad_b = full(2)
    for at, (first, size) in enumerate(tiles):
        span = slice(first, first + size)
        values[:, span] = (dot_nt(grad_b, exit_[span, :]) * slope[:, span]).astype(BF16)
    total = dot(values[...], entry[...])
    for p in range(heads):
        piece = total[:, p * cols : (p + 1) * cols]
        norm_own[p] = piece
        norm_part[p] = piece.astype(BF16)
    norm_copies = exchange(norm_part, norm_land, norm_send, norm_recv, True)
    scaled = total * gain_ref[...].reshape(1, width)
    one_sum = jnp.sum(scaled, axis=-1, keepdims=True)
    centred = (pic[...].astype(F32) - mean_row) * inv_std
    two_sum = jnp.sum(scaled * centred, axis=-1, keepdims=True)
    lane = lax.broadcasted_iota(jnp.int32, (rows, 128), 1)
    sums_part[head] = jnp.where(lane == 0, one_sum, two_sum)
    sums_copies = exchange(sums_part, sums_land, sums_send, sums_recv, False)
    pending.append(norm_copies)
    pending.append(sums_copies)

    text_dir = scatter_sum(3, dirs_copies, dirs_mine)
    grad_text_out = norm_back(text_dir, fulls[0, head], inv_text).astype(BF16)
    last_full = share_start(3, grad_text_out)
    pending.append(last_full)

    arrived(norm_copies)
    arrived(sums_copies)
    grad_normed = norm_own[head]
    sums = sums_part[head]
    for o in range(1, heads):
        source = (head + heads - o) % heads
        grad_normed = grad_normed + norm_land[source].astype(F32)
        sums = sums + sums_land[source]
    mean_one = sums[:, 0:1] * (1.0 / width)
    mean_two = sums[:, 1:2] * (1.0 / width)
    centred = centres[head]
    scaled = grad_normed * gains[head]
    out_rest[...] = inv_std * (scaled - mean_one - centred * mean_two)

    arrived(last_full)
    out_text[...] = dot_nt(full(3), mapping[...])
    for copies in pending:
        finished(copies)


def per_device(pic, cap, gain, entry, exit_, mapping, scale, shift):
    rows, width = pic.shape
    n = lax.axis_size("dp")
    heads = lax.axis_size("mp")
    cols = cap.shape[1]
    share = rows // heads
    hidden = entry.shape[1]
    flipped = entry.T
    anywhere = pl.BlockSpec(memory_space=pl.ANY)
    vmem = pl.BlockSpec(memory_space=pltpu.VMEM)
    smem = pl.BlockSpec(memory_space=pltpu.SMEM)
    dma = pltpu.SemaphoreType.DMA
    go, rest, text = pl.pallas_call(
        functools.partial(body, n, heads),
        out_shape=(
            jax.ShapeDtypeStruct((rows, width), BF16),
            jax.ShapeDtypeStruct((rows, cols), F32),
            jax.ShapeDtypeStruct((rows, mapping.shape[0]), F32),
        ),
        in_specs=[anywhere, anywhere, vmem, anywhere, anywhere, anywhere, smem, smem],
        out_specs=(vmem, vmem, vmem),
        scratch_shapes=[
            pltpu.VMEM(pic.shape, BF16),
            pltpu.VMEM(cap.shape, BF16),
            pltpu.VMEM(flipped.shape, BF16),
            pltpu.VMEM(exit_.shape, BF16),
            pltpu.VMEM(mapping.shape, BF16),
            dma((5,)),
            pltpu.VMEM((rows, width), BF16),
            pltpu.VMEM((rows, hidden), BF16),
            pltpu.VMEM((rows, hidden), F32),
            pltpu.VMEM((rows, n * share), BF16),
            pltpu.VMEM((rows, width), F32),
            pltpu.VMEM((heads, share, width), F32),
            pltpu.VMEM((4, heads, share, width), BF16),
            pltpu.VMEM((4, heads, share, width), BF16),
            pltpu.VMEM((4, heads, share, width), BF16),
            pltpu.VMEM((n, share, width), BF16),
            pltpu.VMEM((n, share, width), BF16),
            pltpu.VMEM((heads, 1, cols), F32),
            pltpu.VMEM((heads, rows, cols), F32),
            pltpu.VMEM((heads, rows, cols), F32),
            pltpu.VMEM((heads, rows, cols), BF16),
            pltpu.VMEM((heads, rows, cols), BF16),
            pltpu.VMEM((heads, rows, 128), F32),
            pltpu.VMEM((heads, rows, 128), F32),
            dma((4, pl.cdiv(width, TILE), heads)),
            dma((4, pl.cdiv(width, TILE), heads)),
            dma((4, heads)),
            dma((4, heads)),
            dma((heads,)),
            dma((heads,)),
            dma((heads,)),
            dma((heads,)),
            dma((2, 2, n // 2)),
            dma((2, 2, n // 2)),
        ],
        compiler_params=pltpu.CompilerParams(
            collective_id=0, has_side_effects=True, vmem_limit_bytes=60 * 2**20
        ),
        name="contrastive",
    )(
        pic,
        cap,
        gain,
        flipped,
        exit_,
        mapping,
        scale.reshape(1, 1),
        shift.reshape(1, 1),
    )
    first = lax.axis_index("mp") * cols
    grad_image = lax.dynamic_slice_in_dim(go, first, cols, 1).astype(F32) + rest
    return grad_image, text


def flipped_bit(index, bit):
    return index + bit * (1 - 2 * ((index // bit) % 2))


def dot_tn(a, b):
    return lax.dot_general(a, b, TN, preferred_element_type=F32)


def split_three(x):
    high = x.astype(BF16)
    rest = x - high.astype(F32)
    middle = rest.astype(BF16)
    return high, middle, (rest - middle.astype(F32)).astype(BF16)


def square_body(
    pic_hbm,
    cap_hbm,
    gain_hbm,
    entry_hbm,
    exit_hbm,
    map_hbm,
    scale_hbm,
    shift_hbm,
    out_image_hbm,
    out_text_hbm,
    scale_ref,
    shift_ref,
    out_image,
    out_text,
    store_sem,
    pic,
    cap,
    gain_ref,
    entry,
    exit_,
    mapping,
    load_sem,
    normed,
    centred_ref,
    values,
    slope,
    t_own,
    t_part,
    t_land,
    i_own,
    i_part,
    i_land,
    tbuf,
    ibuf,
    weights,
    d_own,
    d_near,
    d_part,
    d_through,
    d_land,
    g_part,
    g_land,
    s_own,
    c_part,
    c_land,
    y_part,
    y_land,
    h_part,
    h_land,
    gt_part,
    gt_land,
    n_part,
    n_land,
    send_sem,
    recv_sem,
):
    rows, width = pic.shape
    share = rows // 2
    hidden = exit_.shape[0]
    cols = width // 2
    me = lax.axis_index("dp")
    head = lax.axis_index("mp")
    other = 1 - head
    by_core = {"dp": flipped_bit(me, 1)}
    by_y = {"dp": flipped_bit(me, 2)}
    by_low = {"dp": flipped_bit(me, 4)}
    by_high = {"dp": flipped_bit(me, 8)}
    by_x = {"mp": other}
    own_rows = pl.ds(pl.multiple_of(head * share, 16), share)
    other_rows = pl.ds(pl.multiple_of(other * share, 16), share)
    tiles = [(first, min(TILE, hidden - first)) for first in range(0, hidden, TILE)]
    chunk = share // 3 if share % 48 == 0 else share
    chunks = range(share // chunk)
    spans = [slice(first, min(first + TILE, width)) for first in range(0, width, TILE)]
    x_back = [k % 2 == 0 for k in chunks]
    x_first = [k == 2 for k in chunks]

    def block(ref, at):
        return ref.at[pl.ds(at * share, share)]

    def part(ref, at, k):
        return ref.at[pl.ds(at * share + k * chunk, chunk)]

    def of(at):
        return slice(at * share, (at + 1) * share)

    def lines(at, k):
        return slice(at * share + k * chunk, at * share + (k + 1) * chunk)

    load_count = 0

    def load(src, dst):
        nonlocal load_count
        copy = pltpu.make_async_copy(src, dst, load_sem.at[load_count])
        load_count += 1
        copy.start()
        return copy

    cap_loads = [
        load(cap_hbm.at[other_rows], block(cap, 1)),
        load(map_hbm, mapping),
        load(cap_hbm.at[own_rows], block(cap, 0)),
    ]
    pic_loads = [
        load(pic_hbm.at[own_rows], block(pic, 0)),
        load(pic_hbm.at[other_rows], block(pic, 1)),
        load(gain_hbm, gain_ref),
        load(scale_hbm, scale_ref),
        load(shift_hbm, shift_ref),
    ]
    entry_loads = [
        load(entry_hbm.at[pl.ds(first, size)], entry.at[pl.ds(first, size)]) for first, size in tiles
    ]

    barrier = pltpu.get_barrier_semaphore()
    partners = (by_x, by_y, by_high, by_low, by_core)
    for partner in partners:
        pl.semaphore_signal(barrier, inc=1, device_id=partner, device_id_type=MESH)

    pending = []

    def push(src, dst, partner):
        at = len(pending)
        copy = pltpu.make_async_remote_copy(
            src_ref=src,
            dst_ref=dst,
            send_sem=send_sem.at[at],
            recv_sem=recv_sem.at[at],
            device_id=partner,
            device_id_type=MESH,
        )
        copy.start()
        pending.append(copy)
        return copy

    def arrived(copies):
        for copy in copies:
            copy.wait_recv()

    for copy in cap_loads:
        copy.wait()
    t_part[...] = dot(cap[share:], mapping[...]).astype(BF16)
    pl.semaphore_wait(barrier, len(partners))
    text_partials = [push(part(t_part, 0, k), part(t_land, 0, k), by_x) for k in chunks]
    t_own[...] = dot(cap[:share], mapping[...])
    exit_loads = [
        load(exit_hbm.at[pl.ds(first, size)], exit_.at[pl.ds(first, size)]) for first, size in tiles
    ]

    for copy in pic_loads:
        copy.wait()
    image_float = pic[...].astype(F32)
    mean_row = jnp.mean(image_float, axis=-1, keepdims=True)
    variance = jnp.mean((image_float - mean_row) ** 2, axis=-1, keepdims=True)
    inv_std = lax.rsqrt(variance + 1e-06)
    gain = gain_ref[...].reshape(1, width)
    centred = (image_float - mean_row) * inv_std
    centred_ref[...] = centred
    normed[...] = (centred * gain).astype(BF16)

    def unit_rows(own, land, k, dst):
        total = own[lines(0, k)] + land[lines(0, k)].astype(F32)
        inverse = lax.rsqrt(jnp.sum(total * total, axis=-1, keepdims=True) + 1e-06)
        dst[lines(0, k)] = (total * inverse).astype(BF16)
        return inverse

    inv_text = []
    high_copies = []
    y_copies = []
    early_copies = []
    late_copies = []

    def send_high(k):
        high_copies.append(push(part(tbuf, 0, k), part(tbuf, 4, k), by_high))

    def text_chunk(k):
        text_partials[k].wait_recv()
        inv_text.append(unit_rows(t_own, t_land, k, tbuf))
        if k < 2:
            send_high(k)
        y_copies.append(push(part(tbuf, 0, k), part(tbuf, 1, k), by_y))
        early_copies.append(push(part(tbuf, 0, k), part(tbuf, 2, k), by_core))

    for at, ((first, size), copy) in enumerate(zip(tiles, entry_loads)):
        copy.wait()
        span = slice(first, first + size)
        value, grad = gelu_pair(dot_nt(normed[...], entry[span, :]))
        slope[:, span] = grad
        values[:, span] = value.astype(BF16)
        if at == len(tiles) - 2:
            text_chunk(0)
    for copy in exit_loads:
        copy.wait()
    for span in spans:
        i_part[:, span] = dot(values[share:], exit_[:, span]).astype(BF16)
    image_partials = [push(part(i_part, 0, k), part(i_land, 0, k), by_x) for k in chunks]
    for k in chunks[1:]:
        text_chunk(k)
    for span in spans:
        i_own[:, span] = dot(values[:share], exit_[:, span]) + pic[:share, span].astype(F32)

    inv_image = []
    x_copies = []
    low_copies = []
    for k in chunks:
        image_partials[k].wait_recv()
        inv_image.append(unit_rows(i_own, i_land, k, ibuf))
        x_copies.append(push(part(ibuf, 0, k), part(ibuf, 1, k), by_x))
        low_copies.append(push(part(ibuf, 0, k), part(ibuf, 2, k), by_low))
        if k == 2:
            send_high(2)

    for k in chunks:
        y_copies[k].wait_recv()
        early_copies.append(push(part(tbuf, 1, k), part(tbuf, 3, k), by_core))
    diagonal_copies = []
    image_copies = []
    for k in chunks:
        if x_first[k]:
            x_copies[k].wait_recv()
            image_copies.append(push(part(ibuf, 1, k), part(ibuf, 3, k), by_low))
        else:
            low_copies[k].wait_recv()
            image_copies.append(push(part(ibuf, 2, k), part(ibuf, 3, k), by_x))
        high_copies[k].wait_recv()
        diagonal_copies.append(push(part(tbuf, 4, k), part(tbuf, 5, k), by_y))
        late_copies.append(push(part(tbuf, 4, k), part(tbuf, 6, k), by_core))
    for k in chunks:
        (low_copies if x_first[k] else x_copies)[k].wait_recv()
    arrived(image_copies)
    arrived(early_copies)

    scale = scale_ref[0, 0]
    shift = shift_ref[0, 0]
    early = slice(0, 4 * share)
    late = slice(4 * share, 8 * share)

    def weigh(texts, paired):
        energy = scale * dot_nt(ibuf[...], tbuf[texts, :]) + shift
        if paired:
            row = lax.broadcasted_iota(jnp.int32, energy.shape, 0)
            column = lax.broadcasted_iota(jnp.int32, energy.shape, 1)
            same = jnp.logical_and(row == column, row < share)
            weight = scale * jax.nn.sigmoid(jnp.where(same, -energy, energy))
            weight = jnp.where(same, -weight, weight)
        else:
            weight = scale * jax.nn.sigmoid(energy)
        weights[:, texts] = weight.astype(BF16)

    weigh(early, True)
    c_part[: 2 * share] = dot_tn(weights[:, 2 * share : 4 * share], ibuf[...]).astype(BF16)
    core_early = push(c_part.at[pl.ds(0, 2 * share)], c_land.at[pl.ds(0, 2 * share)], by_core)
    s_own[: 2 * share] = dot_tn(weights[:, : 2 * share], ibuf[...])
    d_near[...] = dot(weights[:, early], tbuf[early, :])

    for k in chunks:
        diagonal_copies[k].wait_recv()
        late_copies.append(push(part(tbuf, 5, k), part(tbuf, 7, k), by_core))
    core_early.wait_recv()
    y_part[of(0), :] = (s_own[of(1), :] + c_land[of(1), :].astype(F32)).astype(BF16)
    s_own[of(0), :] = s_own[of(0), :] + c_land[of(0), :].astype(F32)
    arrived(late_copies)

    weigh(late, False)

    d_part[of(2), :] = (d_near[of(3), :] + dot(weights[of(3), late], tbuf[late, :])).astype(BF16)
    through = [
        push(part(d_part, 2, k), part(d_through, 0, k), by_x if x_back[k] else by_low) for k in chunks
    ]
    d_near[share : 3 * share] += dot(weights[share : 3 * share, late], tbuf[late, :])
    from_x = [None for k in chunks]
    from_low = [None for k in chunks]

    def send_dir(at, k):
        copy = push(part(d_part, at, k), part(d_land, at, k), (by_x, by_low)[at])
        (from_x, from_low)[at][k] = copy

    for k in chunks:
        at = 0 if x_back[k] else 1
        d_part[lines(at, k)] = d_near[lines(at + 1, k)].astype(BF16)
        send_dir(at, k)

    c_part[2 * share :] = dot_tn(weights[:, 6 * share :], ibuf[...]).astype(BF16)
    core_late = [push(block(c_part, at), block(c_land, at), by_core) for at in (3, 2)]
    s_own[2 * share :] = dot_tn(weights[:, 4 * share : 6 * share], ibuf[...])
    core_late[0].wait_recv()
    y_part[of(1), :] = (s_own[of(3), :] + c_land[of(3), :].astype(F32)).astype(BF16)
    diagonal_copies = [push(part(y_part, 1, k), part(y_land, 1, k), by_y) for k in chunks]
    y_copies = [push(part(y_part, 0, k), part(y_land, 0, k), by_y) for k in chunks]
    for k in chunks:
        at = 1 if x_back[k] else 0
        through[k].wait_recv()
        total = d_near[lines(at + 1, k)] + d_through[lines(0, k)].astype(F32)
        d_part[lines(at, k)] = total.astype(BF16)
        send_dir(at, k)
    d_own[...] = d_near[of(0), :] + dot(weights[of(0), late], tbuf[late, :])
    core_late[1].wait_recv()
    s_own[of(2), :] = s_own[of(2), :] + c_land[of(2), :].astype(F32)
    high_copies = []
    for k in chunks:
        diagonal_copies[k].wait_recv()
        h_part[lines(0, k)] = (s_own[lines(2, k)] + y_land[lines(1, k)].astype(F32)).astype(BF16)
        high_copies.append(push(part(h_part, 0, k), part(h_land, 0, k), by_high))

    grad_copies = []
    for k in chunks:
        from_x[k].wait_recv()
        from_low[k].wait_recv()
        total = d_own[lines(0, k)] + d_land[lines(0, k)].astype(F32) + d_land[lines(1, k)].astype(F32)
        g_part[lines(0, k)] = norm_back(total, ibuf[lines(0, k)], inv_image[k]).astype(BF16)
        grad_copies.append(push(part(g_part, 0, k), part(g_land, 0, k), by_x))

    gain = gain_ref[...].reshape(1, width)
    mine_first = head == 0
    gains = jnp.where(mine_first, gain[:, :cols], gain[:, cols:])
    stores = []

    def store(src, dst, first, begin, count):
        start = pl.multiple_of(begin, 16)
        copy = pltpu.make_async_copy(
            src.at[pl.ds(first, count)], dst.at[pl.ds(start, count)], store_sem.at[len(stores)]
        )
        copy.start()
        stores.append(copy)

    def backward_exit(at, upstream):
        grad_b = upstream[...]
        for begin, size in tiles:
            span = slice(begin, begin + size)
            values[of(at), span] = (dot_nt(grad_b, exit_[span, :]) * slope[of(at), span]).astype(BF16)

    def backward_entry(at):
        total = dot(values[of(at), :], entry[...])
        lower = total[:, :cols]
        upper = total[:, cols:]
        n_part[of(at), :cols] = jnp.where(mine_first, upper, lower).astype(BF16)
        grad_normed = jnp.where(mine_first, lower, upper)
        scaled = total * gain
        one_sum = jnp.sum(scaled, axis=-1, keepdims=True)
        two_sum = jnp.sum(scaled * centred_ref[of(at), :], axis=-1, keepdims=True)
        lane = lax.broadcasted_iota(jnp.int32, (share, n_part.shape[1] - cols), 1)
        packed = jnp.zeros(lane.shape, F32)
        for place, term in enumerate(split_three(one_sum) + split_three(two_sum)):
            packed = jnp.where(lane == place, term.astype(F32), packed)
        n_part[of(at), cols:] = packed.astype(BF16)
        return push(block(n_part, at), block(n_land, 1 - at), by_x), (grad_normed, one_sum, two_sum)

    def finish(at, upstream, grad_normed, one_sum, two_sum):
        lines = of(at)
        grad_float = upstream[...].astype(F32)
        grad_float = jnp.where(mine_first, grad_float[:, :cols], grad_float[:, cols:])
        centred = centred_ref[lines, :]
        centred = jnp.where(mine_first, centred[:, :cols], centred[:, cols:])
        grad_normed = grad_normed + n_land[lines, :cols].astype(F32)
        sums = n_land[lines, cols:].astype(F32)
        mean_one = (one_sum + (sums[:, 0:1] + sums[:, 1:2] + sums[:, 2:3])) * (1.0 / width)
        mean_two = (two_sum + (sums[:, 3:4] + sums[:, 4:5] + sums[:, 5:6])) * (1.0 / width)
        result = grad_float + inv_std[lines] * (grad_normed * gains - mean_one - centred * mean_two)
        out_image[lines, :] = result
        store(out_image, out_image_hbm, at * share, (head, other)[at] * share, share)

    text_copies = []

    def text_back(k):
        high_copies[k].wait_recv()
        y_copies[k].wait_recv()
        total = s_own[lines(0, k)] + y_land[lines(0, k)].astype(F32) + h_land[lines(0, k)].astype(F32)
        gt_part[lines(0, k)] = norm_back(total, tbuf[lines(0, k)], inv_text[k]).astype(BF16)
        text_copies.append(push(part(gt_part, 0, k), part(gt_land, 0, k), by_x))

    backward_exit(0, g_part)
    own_copy, own_terms = backward_entry(0)
    arrived(grad_copies)
    backward_exit(1, g_land)
    text_back(0)
    their_copy, their_terms = backward_entry(1)
    for k in chunks[1:]:
        text_back(k)
    own_copy.wait_recv()
    finish(1, g_land, *their_terms)
    out_text[:share, :] = dot_nt(gt_part[...], mapping[...])
    store(out_text, out_text_hbm, 0, head * share, share)
    their_copy.wait_recv()
    finish(0, g_part, *own_terms)
    arrived(text_copies)
    out_text[share:, :] = dot_nt(gt_land[...], mapping[...])
    store(out_text, out_text_hbm, share, other * share, share)
    for copy in pending:
        copy.wait_send()
    for copy in stores:
        copy.wait()


def hand_over(image_hbm, text_hbm, out_image, out_text, image, text, in_sem, out_sem):
    rows = image.shape[0]
    count = 4 if rows % 32 == 0 else 1
    size = rows // count
    pieces = [
        (src, mid, dst, pl.ds(at * size, size))
        for at in range(count)
        for src, mid, dst in ((image_hbm, image, out_image), (text_hbm, text, out_text))
    ]
    ins = []
    outs = []
    for at, (src, mid, dst, lines) in enumerate(pieces):
        ins.append(pltpu.make_async_copy(src.at[lines], mid.at[lines], in_sem.at[at]))
        outs.append(pltpu.make_async_copy(mid.at[lines], dst.at[lines], out_sem.at[at]))
        ins[at].start()
    for taken, given in zip(ins, outs):
        taken.wait()
        given.start()
    for given in outs:
        given.wait()


def square_device(pic, cap, gain, entry, exit_, mapping, scale, shift):
    rows, width = pic.shape
    cols = cap.shape[1]
    share = rows // 2
    hidden = entry.shape[1]
    flipped = entry.T
    anywhere = pl.BlockSpec(memory_space=pl.ANY)
    dma = pltpu.SemaphoreType.DMA

    def blocks(count, dtype=BF16):
        return pltpu.VMEM((count * share, width), dtype)

    loads = 8 + 2 * pl.cdiv(hidden, TILE)
    copies = 66
    extended = 128 * (cols // 128 + 1)
    results = (
        jax.ShapeDtypeStruct((rows, cols), F32),
        jax.ShapeDtypeStruct((rows, mapping.shape[0]), F32),
    )
    image, text = pl.pallas_call(
        square_body,
        out_shape=results,
        in_specs=[anywhere] * 8,
        out_specs=(anywhere, anywhere),
        scratch_shapes=[
            pltpu.SMEM((1, 1), F32),
            pltpu.SMEM((1, 1), F32),
            pltpu.VMEM((rows, cols), F32),
            pltpu.VMEM((rows, mapping.shape[0]), F32),
            dma((4,)),
            pltpu.VMEM(pic.shape, BF16),
            pltpu.VMEM(cap.shape, BF16),
            pltpu.VMEM(gain.shape, F32),
            pltpu.VMEM(flipped.shape, BF16),
            pltpu.VMEM(exit_.shape, BF16),
            pltpu.VMEM(mapping.shape, BF16),
            dma((loads,)),
            pltpu.VMEM((rows, width), BF16),
            pltpu.VMEM((rows, width), F32),
            pltpu.VMEM((rows, hidden), BF16),
            pltpu.VMEM((rows, hidden), F32),
            blocks(1, F32),
            blocks(1),
            blocks(1),
            blocks(1, F32),
            blocks(1),
            blocks(1),
            blocks(8),
            blocks(4),
            pltpu.VMEM((4 * share, 8 * share), BF16),
            blocks(1, F32),
            blocks(4, F32),
            blocks(3),
            blocks(1),
            blocks(2),
            blocks(1),
            blocks(1),
            blocks(4, F32),
            blocks(4),
            blocks(4),
            blocks(2),
            blocks(2),
            blocks(1),
            blocks(1),
            blocks(1),
            blocks(1),
            pltpu.VMEM((rows, extended), BF16),
            pltpu.VMEM((rows, extended), BF16),
            dma((copies,)),
            dma((copies,)),
        ],
        compiler_params=pltpu.CompilerParams(
            collective_id=0, has_side_effects=True, vmem_limit_bytes=60 * 2**20
        ),
        name="contrastive_square",
    )(
        pic,
        cap,
        gain,
        flipped,
        exit_,
        mapping,
        scale.reshape(1, 1),
        shift.reshape(1, 1),
    )
    return pl.pallas_call(
        hand_over,
        out_shape=results,
        in_specs=[anywhere, anywhere],
        out_specs=(anywhere, anywhere),
        scratch_shapes=[pltpu.VMEM(r.shape, F32) for r in results] + [dma((8,)), dma((8,))],
        compiler_params=pltpu.CompilerParams(vmem_limit_bytes=60 * 2**20),
        name="hand_over",
    )(image, text)


def solution(mesh):
    in_specs = (
        P("dp", None),
        P("dp", "mp"),
        P(),
        P(None, "mp"),
        P("mp", None),
        P("mp", None),
        P(),
        P(),
    )
    out_specs = (P("dp", "mp"), P("dp", "mp"))
    square = mesh.shape["mp"] == 2 and mesh.shape["dp"] == 16
    return jax.shard_map(
        square_device if square else per_device, mesh=mesh, in_specs=in_specs, out_specs=out_specs, check_vma=False
    )
```
